256 devices in a mesh: seq: 64 (over x, z, core), head: 4 (over y).
Axes of the slice: x: 4, y: 4, z: 8, core: 2. Of those that a mesh axis runs over, the one named last changes fastest.
Arguments:
- stream: bfloat16 [32768, 5120], P('seq', 'head'), may hold values from -6 to 6
- gate_input: bfloat16 [32768, 5120], P('seq', 'head'), may hold values from -6 to 6
- in_coeff: bfloat16 [32768, 128], P('seq'), may hold values from -0.5 to 0.5
- out_coeff: bfloat16 [32768, 128], P('seq'), may hold values from -0.5 to 0.5
- step_raw: float32 [80, 32768], P('head', 'seq'), may hold values from -4 to 4
- step_bias: float32 [80], P('head'), may hold values from -1 to 1
- decay_rate: float32 [80], P('head'), may hold values from 3.0517578e-05 to 0.05
- skip_scale: float32 [80], P('head'), may hold values from 0.5 to 5
- norm_gain: float32 [5120], P('head'), may hold values from 0.1 to 1.9
- out_proj: bfloat16 [5120, 2560], P('head'), may hold values from -0.078125 to 0.078125
- doc_starts: int32 [128], replicated, may hold values from 0 to 32767, as said below
Outputs:
- layer_out: bfloat16 [32768, 2560], P(('seq', 'head'))
The draws below stay inside these ranges and needn't reach their ends.
Inputs may be any that keep to these rules, and one draw needn't show every extreme that they name: `doc_starts`: the first entry is 0, the last is 32767, and the entries strictly increase; entry i is the position where document i begins.
All inputs are finite; a program needn't handle non-finite values.
Results may differ from the reference program's by a relative error of at most 0.01.
Values may be sent and summed in bfloat16 or wider, within the bound.
A program may use at most 128 MiB of HBM per device.

```python
import math
import jax
import jax.numpy as jnp
from jax import lax

D = 2560
HEADS = 80
HEAD_DIM = 64
STATE = 128
DI = 5120
BLOCK = 256
TOKENS = 32768
DOCS = 128
N_HEAD = 4


def draw_decay_rate(key, part):
    pick_key = jax.random.fold_in(key, 101)
    slow_key = jax.random.fold_in(key, 102)
    fast_key = jax.random.fold_in(key, 103)
    slow_share = 0.5
    slow_pick = jax.random.uniform(pick_key, (HEADS,), jnp.float32) < slow_share
    slow_rate = jnp.exp(jax.random.uniform(slow_key, (HEADS,), jnp.float32, 0.0, math.log(2.5))) / TOKENS
    fast_rate = jnp.exp(jax.random.uniform(fast_key, (HEADS,), jnp.float32, math.log(0.01), math.log(0.05)))
    return jnp.where(slow_pick, slow_rate, fast_rate).astype(jnp.float32)


def draw_skip_scale(key, part):
    noise_key = jax.random.fold_in(key, 201)
    ramp_line = 1.0 + 2.0 * jnp.arange(HEADS, dtype=jnp.float32) / max(HEADS - 1, 1)
    noise = jax.random.uniform(noise_key, (HEADS,), jnp.float32, 0.6, 1.4)
    return (ramp_line * noise).astype(jnp.float32)


def draw_doc_starts(key, part):
    quarter_span = TOKENS // 4
    cut_key = jax.random.fold_in(key, 301)
    shuffled = jax.random.permutation(cut_key, quarter_span) + quarter_span
    cuts = jnp.sort(shuffled[:DOCS - 2]).astype(jnp.int32)
    first_one = jnp.zeros((1,), jnp.int32)
    last_one = jnp.full((1,), TOKENS - 1, jnp.int32)
    return jnp.concatenate([first_one, cuts, last_one]).astype(jnp.int32)


def block_scale(key, dims, shards, least, top_value):
    def one(axis_at, blocks):
        heights = jax.random.uniform(jax.random.fold_in(jax.random.fold_in(key, 6), axis_at), (blocks,), jnp.float32, least / len(shards), top_value / len(shards))
        return jnp.repeat(jnp.exp(heights), dims[axis_at] // blocks).reshape((-1,) + (1,) * (len(dims) - axis_at - 1))

    level = one(*shards[0])
    for cut in shards[1:]:
        level = level * one(*cut)
    return level


def gaussian(key, extent, spread, limit, cuts=(), held_as=jnp.bfloat16):
    array = spread * jax.random.normal(key, extent, jnp.float32)
    if cuts:
        array = array * block_scale(key, extent, cuts, -0.22, 0.18)
    return jnp.clip(array, -limit, limit).astype(held_as)


def setup_inputs(seed: int = 0) -> dict:
    key_list = jax.random.split(jax.random.key(seed), 12)
    return {
        "stream": gaussian(key_list[0], (TOKENS, DI), 1.0, 6.0, ((0, 64), (1, 4))),
        "gate_input": gaussian(key_list[1], (TOKENS, DI), 1.0, 6.0, ((0, 64), (1, 4))),
        "in_coeff": gaussian(key_list[2], (TOKENS, STATE), STATE ** -0.5, 0.5, ((0, 64),)),
        "out_coeff": gaussian(key_list[3], (TOKENS, STATE), STATE ** -0.5, 0.5, ((0, 64),)),
        "step_raw": gaussian(key_list[4], (HEADS, TOKENS), 1.0, 4.0, ((0, 4), (1, 64)), jnp.float32),
        "step_bias": jnp.clip(jax.random.uniform(key_list[5], (HEADS,), jnp.float32, -1.0, 1.0) * block_scale(key_list[5], (HEADS,), ((0, 4),), -0.4, 0.0), -1.0, 1.0),
        "decay_rate": draw_decay_rate(jax.random.fold_in(key_list[11], 71), 0),
        "skip_scale": draw_skip_scale(jax.random.fold_in(key_list[11], 71), 0),
        "norm_gain": jnp.clip(1.0 + 0.18 * jax.random.normal(key_list[8], (DI,), jnp.float32), 0.1, 1.9),
        "out_proj": gaussian(key_list[9], (DI, D), DI ** -0.5, 0.078125, ((0, 4),)),
        "doc_starts": draw_doc_starts(jax.random.fold_in(key_list[11], 71), 0),
    }


EPSILON = 1e-05
HIGHEST = lax.Precision.HIGHEST

def block_pass(carry_state, block_piece):
    stream_blk, in_blk, out_blk, step_blk, log_blk, doc_blk, before = block_piece
    head_count = step_blk.shape[0]
    span = step_blk.shape[1]
    head_size = stream_blk.shape[1] // head_count
    index_row = lax.iota(jnp.int32, span)
    upper_ones = (index_row[:, None] <= index_row[None, :]).astype(jnp.float32)
    cumulative = jnp.dot(log_blk, upper_ones, precision=HIGHEST)
    last_cum = cumulative[:, -1]
    same_end = (doc_blk == doc_blk[-1]).astype(jnp.float32)
    end_weight = jnp.exp(jnp.minimum(last_cum[:, None] - cumulative, 0.0)) * step_blk * same_end[None, :]
    scaled_in = (end_weight[:, :, None] * in_blk.astype(jnp.float32)[None, :, :]).astype(jnp.bfloat16)
    values = stream_blk.reshape(span, head_count, head_size)
    fresh_state = jnp.einsum('hsn,shp->hnp', scaled_in.astype(jnp.float32), values.astype(jnp.float32), precision=HIGHEST)
    joined = doc_blk == before
    carry_gate = jnp.where(joined[-1], jnp.exp(last_cum), 0.0)
    new_state = carry_gate[:, None, None] * carry_state + fresh_state
    scores = jnp.dot(out_blk, in_blk.T, preferred_element_type=jnp.float32)
    live_pairs = (doc_blk[:, None] == doc_blk[None, :]) & (index_row[:, None] >= index_row[None, :])
    decay_pairs = jnp.where(live_pairs[None], jnp.exp(jnp.minimum(cumulative[:, :, None] - cumulative[:, None, :], 0.0)), 0.0)
    weights = (scores[None] * decay_pairs * step_blk[:, None, :]).astype(jnp.bfloat16)
    within = jnp.einsum('hts,shp->thp', weights.astype(jnp.float32), values.astype(jnp.float32), precision=HIGHEST)
    carried = jnp.einsum('tn,hnp->thp', out_blk.astype(jnp.float32), carry_state, precision=HIGHEST)
    factor = jnp.where(joined[None, :], jnp.exp(cumulative), 0.0)
    output = within + factor.T[:, :, None] * carried
    return (new_state, output)

def reference(stream, gate_input, in_coeff, out_coeff, step_raw, step_bias, decay_rate, skip_scale, norm_gain, out_proj, doc_starts):
    position = lax.iota(jnp.int32, TOKENS)
    doc_ids = lax.optimization_barrier(jnp.sum((doc_starts[None, :] <= position[:, None]).astype(jnp.int32), axis=1)) - 1
    step_size = jax.nn.softplus(step_raw + step_bias[:, None])
    log_decay = -step_size * decay_rate[:, None]
    block_count = TOKENS // BLOCK
    block_docs = doc_ids.reshape(block_count, BLOCK)
    block_before = jnp.concatenate([jnp.full((1,), -1, jnp.int32), block_docs[:-1, -1]])
    pieces = (stream.reshape(block_count, BLOCK, DI), in_coeff.reshape(block_count, BLOCK, STATE), out_coeff.reshape(block_count, BLOCK, STATE), step_size.reshape(HEADS, block_count, BLOCK).transpose(1, 0, 2), log_decay.reshape(HEADS, block_count, BLOCK).transpose(1, 0, 2), block_docs, block_before)
    zero_state = jnp.zeros((HEADS, STATE, HEAD_DIM), jnp.float32)
    last_state, outputs = lax.scan(block_pass, zero_state, pieces)
    ssm_out = outputs.reshape(TOKENS, HEADS, HEAD_DIM) + skip_scale[None, :, None] * stream.reshape(TOKENS, HEADS, HEAD_DIM).astype(jnp.float32)
    gated = ssm_out.reshape(TOKENS, DI) * jax.nn.silu(gate_input.astype(jnp.float32))
    scale_row = lax.rsqrt(lax.optimization_barrier(jnp.sum(gated * gated, axis=1)) / DI + EPSILON)
    hidden = (gated * scale_row[:, None] * norm_gain[None, :]).astype(jnp.bfloat16)
    group_width = DI // N_HEAD
    summed = jnp.zeros((TOKENS, D), jnp.float32)
    for group_index in range(N_HEAD):
        low = group_index * group_width
        part_sum = jnp.dot(hidden[:, low:low + group_width], out_proj[low:low + group_width, :], preferred_element_type=jnp.float32)
        summed = summed + lax.optimization_barrier(part_sum.astype(jnp.bfloat16)).astype(jnp.float32)
    return summed.astype(jnp.bfloat16)
```

```python
import functools

import jax
import jax.numpy as jnp
from jax import lax
from jax.experimental import pallas as pl
from jax.experimental.pallas import tpu as pltpu
from jax.sharding import PartitionSpec as P

DI = 5120
EPSILON = 1e-05
ROW = 16
LANE = 128
F32 = jnp.float32
BF16 = jnp.bfloat16
MESH = pl.DeviceIdType.MESH


def dot(a, b):
    return jnp.dot(a, b, preferred_element_type=F32)


def dot_nt(a, b):
    return lax.dot_general(a, b, (((1,), (1,)), ((), ())), preferred_element_type=F32)


def rounded(v):
    return v.astype(BF16).astype(F32)


def eye_mask(n):
    return lax.broadcasted_iota(jnp.int32, (n, n), 0) == lax.broadcasted_iota(jnp.int32, (n, n), 1)


def as_column(row, n):
    return jnp.sum(jnp.where(eye_mask(n), row, 0.0), axis=1, keepdims=True)


def as_row(column, n):
    return jnp.sum(jnp.where(eye_mask(n), column, 0.0), axis=0, keepdims=True)


def link_tile(row, rows):
    high = rounded(row)
    middle = rounded(row - high)
    low = row - high - middle
    at = lax.broadcasted_iota(jnp.int32, (rows, LANE), 0)
    return jnp.where(
        at == 0, high, jnp.where(at == 1, middle, jnp.where(at == 2, low, 0.0))
    ).astype(BF16)


def kernel(
    nx,
    nr,
    ny,
    x_hbm,
    g_hbm,
    b_hbm,
    c_hbm,
    st_hbm,
    bias_ref,
    rate_ref,
    skip_ref,
    gain_ref,
    w_hbm,
    doc_ref,
    out_ref,
    x_v,
    g_v,
    b_v,
    c_v,
    st_v,
    w_v,
    m_ref,
    mt_ref,
    e_ref,
    v_ref,
    sc_ref,
    cj_ref,
    a1_ref,
    a2_ref,
    row_ref,
    asend,
    arecv,
    ll_ref,
    lx_ref,
    pre_ref,
    pl_ref,
    xsend,
    xrecv,
    bsend,
    brecv,
    sp_ref,
    hid_ref,
    r1_send,
    r1_recv,
    r2_send,
    r2_recv,
    own_ref,
    ss_send,
    ss_recv,
    copy_sem,
    a_ssem,
    a_rsem,
    x_ssem,
    x_rsem,
    b_ssem,
    b_rsem,
    r1_ssem,
    r1_rsem,
    r2_ssem,
    r2_rsem,
    ss_ssem,
    ss_rsem,
):
    seq = lax.axis_index("seq")
    head = lax.axis_index("head")
    xi = seq // nr
    me = seq % nr
    tokens, channels = x_v.shape
    heads = st_v.shape[0]
    state = b_v.shape[1]
    width = w_v.shape[1]
    half = width // 2
    sr = state // nr
    part = tokens // ny
    offset = seq * tokens
    head_size = channels // heads

    loads = [
        pltpu.make_async_copy(src, dst, copy_sem.at[i])
        for i, (src, dst) in enumerate(
            (
                (st_hbm, st_v),
                (b_hbm, b_v),
                (x_hbm, x_v),
                (c_hbm, c_v),
                (g_hbm, g_v),
                (w_hbm, w_v),
            )
        )
    ]
    for load in loads:
        load.start()

    barrier = pltpu.get_barrier_semaphore()
    in_row = [(xi * nr + (me + k) % nr, head) for k in range(nr)]
    in_x = [(((xi + k) % nx) * nr + me, head) for k in range(nx)]
    in_y = [(seq, (head + k) % ny) for k in range(ny)]
    for device in in_row[1:] + in_x[1:] + in_y[1:]:
        pl.semaphore_signal(barrier, inc=1, device_id=device, device_id_type=MESH)

    e_ref[...] = (
        (lax.broadcasted_iota(jnp.int32, (LANE, channels), 0) & 31)
        == lax.broadcasted_iota(jnp.int32, (LANE, channels), 1) // head_size
    ).astype(F32).astype(BF16)
    m_ref[...] = jnp.zeros_like(m_ref)
    starts = doc_ref[...]
    position = offset + lax.broadcasted_iota(jnp.int32, (tokens, 1), 0)
    doc_start = jnp.max(
        jnp.where(starts <= position, starts.astype(F32), -1.0), axis=1, keepdims=True
    )
    joined = doc_start < offset.astype(F32)
    last_start = doc_start[tokens - 1 :, :]

    bias = as_column(bias_ref[...], heads)
    rate = as_column(rate_ref[...], heads)
    skip = as_column(skip_ref[...], heads)
    loads[0].wait()
    step = st_v[...] + bias
    step = jnp.maximum(step, 0.0) + jnp.log1p(jnp.exp(-jnp.abs(step)))
    cum = -step * rate
    lane = lax.broadcasted_iota(jnp.int32, (heads, tokens), 1)
    shift = 1
    while shift < tokens:
        cum = cum + jnp.where(lane >= shift, pltpu.roll(cum, shift, 1), 0.0)
        shift *= 2
    mid = cum[:, tokens // 2 - 1 : tokens // 2]
    total = cum[:, tokens - 1 :]
    before_scale = jnp.exp(mid - cum) * step
    after_scale = jnp.exp(cum - mid)

    def put(first, columns, value):
        high = rounded(value)
        m_ref[first : first + heads, columns] = high
        m_ref[first + 32 : first + 32 + heads, columns] = value - high

    wide = (heads, LANE)
    put(0, slice(0, tokens), before_scale)
    put(64, slice(0, tokens), after_scale)
    put(0, slice(tokens, tokens + LANE), jnp.broadcast_to(jnp.exp(mid), wide))
    put(64, slice(tokens, tokens + LANE), jnp.broadcast_to(skip, wide))
    mt_ref[...] = m_ref[...].T.astype(BF16)
    gate_row = jnp.where(last_start < offset.astype(F32), total, -1e30)
    link_row = jnp.sum(
        jnp.where(
            lax.broadcasted_iota(jnp.int32, (heads, LANE), 0)
            == lax.broadcasted_iota(jnp.int32, (heads, LANE), 1),
            gate_row,
            0.0,
        ),
        axis=0,
        keepdims=True,
    )

    def expand(rows, upper):
        block = mt_ref[rows, :]
        at = lax.broadcasted_iota(jnp.int32, block.shape, 1)
        block = jnp.where((at >= 64) if upper else (at < 64), block.astype(F32), 0.0)
        return block.astype(BF16)

    row_ref[0:8, :] = dot(expand(slice(tokens - 8, tokens), True), e_ref[...])
    row_ref[8:16, :] = dot(expand(slice(tokens, tokens + 8), False), e_ref[...])
    row_ref[16:24, :] = dot(expand(slice(tokens, tokens + 8), True), e_ref[...])

    loads[2].wait()
    step_rows = 128
    columns = [slice(c, c + 256) for c in range(0, channels, 256)]

    @pl.loop(0, tokens // step_rows)
    def _(i):
        rows = pl.ds(pl.multiple_of(i * step_rows, step_rows), step_rows)
        left = expand(rows, False)
        for cols in columns:
            v_ref[rows, cols] = (
                x_v[rows, cols].astype(F32) * dot(left, e_ref[:, cols])
            ).astype(BF16)

    loads[1].wait()
    kept = jnp.where(position.astype(F32) >= last_start, b_v[...].astype(F32), 0.0)
    kept = kept.T.astype(BF16)
    tile = link_tile(link_row, sr)
    for cols in columns:
        piece = dot(kept, v_ref[:, cols]) * row_ref[7:8, cols]
        for j in range(nr):
            asend[j, :, cols] = piece[j * sr : (j + 1) * sr, :].astype(BF16)
    for j in range(nr):
        asend[j, :, channels:] = tile

    pl.semaphore_wait(barrier, nr + nx + ny - 3)

    def around(n):
        order = []
        for d in range(n // 2, 0, -1):
            order += [d] if 2 * d == n else [d, n - d]
        return order

    row_copies = {}
    for k in around(nr):
        target = (me + k) % nr
        row_copies[k] = pltpu.make_async_remote_copy(
            src_ref=asend.at[target],
            dst_ref=arecv.at[me],
            send_sem=a_ssem.at[k - 1],
            recv_sem=a_rsem.at[k - 1],
            device_id=in_row[k],
            device_id_type=MESH,
        )
        row_copies[k].start()
    arecv[me] = asend[me]

    loads[3].wait()
    cj_ref[...] = jnp.where(joined, c_v[...].astype(F32), 0.0).astype(BF16)
    loads[4].wait()

    @pl.loop(0, tokens // step_rows)
    def _(i):
        first = pl.multiple_of(i * step_rows, step_rows)
        rows = pl.ds(first, step_rows)
        scores = dot_nt(c_v[rows, :], b_v[...])
        at = offset + first + lax.broadcasted_iota(jnp.int32, (step_rows, 1), 0)
        source = offset + lax.broadcasted_iota(jnp.int32, (step_rows, tokens), 1)
        begun = jnp.max(
            jnp.where(starts <= at, starts.astype(F32), -1.0), axis=1, keepdims=True
        )
        live = (source <= at) & (source.astype(F32) >= begun)
        sc_ref[...] = jnp.where(live, scores, 0.0).astype(BF16)
        left = expand(rows, True)
        for cols in columns:
            scale = dot(left, e_ref[:, cols])
            gate = g_v[rows, cols].astype(F32)
            gate = gate / (1.0 + jnp.exp(-gate))
            inside = dot(sc_ref[...], v_ref[:, cols])
            skipped = row_ref[16:17, cols] * x_v[rows, cols].astype(F32)
            a1_ref[rows, cols] = scale * gate
            a2_ref[rows, cols] = (scale * inside + skipped) * gate

    for k in around(nr):
        row_copies[k].wait_recv()

    def link_of(block):
        pieces = block[:, channels:].astype(F32)
        return jnp.sum(pieces, axis=0, keepdims=True)

    def spread(logs):
        at = lax.broadcasted_iota(jnp.int32, logs.shape, 1)
        value = jnp.where(at < heads, jnp.exp(logs), 0.0)
        high = value.astype(BF16)
        rest = value - high.astype(F32)
        middle = rest.astype(BF16)
        low = (rest - middle.astype(F32)).astype(BF16)
        return dot(high, e_ref[...]) + dot(middle, e_ref[...]) + dot(low, e_ref[...])

    for j in range(nr):
        ll_ref[j : j + 1, :] = link_of(arecv[j])
    row_log = jnp.sum(ll_ref[0:nr, :], axis=0, keepdims=True)
    lx_ref[0:nr, :] = spread(ll_ref[0:nr, :])
    prefix = jnp.zeros((sr, channels), F32)
    product = jnp.ones((1, channels), F32)
    for j in range(nr):
        pre_ref[j] = prefix
        pl_ref[j : j + 1, :] = product
        link = lx_ref[j : j + 1, :]
        prefix = link * prefix + arecv[j, :, 0:channels].astype(F32)
        product = product * link
    xsend[:, 0:channels] = prefix.astype(BF16)
    xsend[:, channels:] = link_tile(row_log, sr)

    x_copies = {}
    for k in around(nx):
        x_copies[k] = pltpu.make_async_remote_copy(
            src_ref=xsend,
            dst_ref=xrecv.at[xi],
            send_sem=x_ssem.at[k - 1],
            recv_sem=x_rsem.at[k - 1],
            device_id=in_x[k],
            device_id_type=MESH,
        )
        x_copies[k].start()
    xrecv[xi] = xsend[...]
    for k in around(nx):
        x_copies[k].wait_recv()
    for j in range(nx):
        ll_ref[j : j + 1, :] = link_of(xrecv[j])
    lx_ref[0:nx, :] = spread(ll_ref[0:nx, :])
    earlier = jnp.zeros((sr, channels), F32)
    for j in range(nx - 1):
        after = lx_ref[j : j + 1, :] * earlier + xrecv[j, :, 0:channels].astype(F32)
        earlier = jnp.where(j < xi, after, earlier)
    for j in range(nr):
        bsend[j] = (pre_ref[j] + pl_ref[j : j + 1, :] * earlier).astype(BF16)

    back_copies = {}
    for k in around(nr):
        target = (me + k) % nr
        back_copies[k] = pltpu.make_async_remote_copy(
            src_ref=bsend.at[target],
            dst_ref=brecv.at[me],
            send_sem=b_ssem.at[k - 1],
            recv_sem=b_rsem.at[k - 1],
            device_id=in_row[k],
            device_id_type=MESH,
        )
        back_copies[k].start()
    brecv[me] = bsend[me]
    for k in around(nr):
        back_copies[k].wait_recv()
    for j in range(nr):
        rows = slice(j * sr, (j + 1) * sr)
        sp_ref[rows, :] = (row_ref[8:9, :] * brecv[j].astype(F32)).astype(BF16)

    sends = [*row_copies.values(), *x_copies.values(), *back_copies.values()]

    def make_hidden(k):
        chunk = (head + k) % ny
        rows = pl.ds(pl.multiple_of(chunk * part, part), part)
        squares = jnp.zeros((part, 1), F32)
        for cols in columns:
            gated = a2_ref[rows, cols] + a1_ref[rows, cols] * dot(
                cj_ref[rows, :], sp_ref[:, cols]
            )
            squares = squares + jnp.sum(gated * gated, axis=1, keepdims=True)
            hid_ref[rows, cols] = (gated * gain_ref[:, cols]).astype(BF16)
        ss_send[k] = jnp.broadcast_to(as_row(squares, part), (8, part))
        if k:
            copy = pltpu.make_async_remote_copy(
                src_ref=ss_send.at[k],
                dst_ref=ss_recv.at[k - 1],
                send_sem=ss_ssem.at[k - 1],
                recv_sem=ss_rsem.at[k - 1],
                device_id=in_y[k],
                device_id_type=MESH,
            )
            copy.start()
            return copy

    def project(k, side, store):
        chunk = (head + k) % ny
        rows = pl.ds(pl.multiple_of(chunk * part, part), part)
        for c in range(0, half, 256):
            store(
                slice(c, c + 256),
                dot(hid_ref[rows, :], w_v[:, side * half + c : side * half + c + 256]),
            )

    def send(src, dst, ssem, rsem, device):
        copy = pltpu.make_async_remote_copy(
            src_ref=src,
            dst_ref=dst,
            send_sem=ssem,
            recv_sem=rsem,
            device_id=device,
            device_id_type=MESH,
        )
        copy.start()
        return copy

    def into(ref):
        def store(cols, value):
            ref[:, cols] = value.astype(BF16)

        return store

    def added(ref, extra):
        def store(cols, value):
            ref[:, cols] = (value + extra[:, cols].astype(F32)).astype(BF16)

        return store

    up, down = in_y[1], in_y[ny - 1]
    squares_sent = [make_hidden(2)]
    loads[5].wait()
    first = []
    for side, device in ((0, up), (1, down)):
        project(2, side, into(r1_send.at[side]))
        first.append(
            send(
                r1_send.at[side],
                r1_recv.at[side],
                r1_ssem.at[side],
                r1_rsem.at[side],
                device,
            )
        )
    second = []
    for side, k, device in ((0, 1, up), (1, ny - 1, down)):
        squares_sent.append(make_hidden(k))
        project(k, 1 - side, into(r2_send.at[side, 0]))
        second.append(
            send(
                r2_send.at[side, 0],
                r2_recv.at[side, 0],
                r2_ssem.at[side, 0],
                r2_rsem.at[side, 0],
                device,
            )
        )
    make_hidden(0)
    for side in (0, 1):

        def store(cols, value, side=side):
            own_ref[:, side * half + cols.start : side * half + cols.stop] = value

        project(0, side, store)
    for side, k, device in ((0, 1, up), (1, ny - 1, down)):
        first[side].wait_recv()
        project(k, side, added(r2_send.at[side, 1], r1_recv.at[side]))
        second.append(
            send(
                r2_send.at[side, 1],
                r2_recv.at[side, 1],
                r2_ssem.at[side, 1],
                r2_rsem.at[side, 1],
                device,
            )
        )
    for copy in squares_sent:
        copy.wait_recv()
    total_squares = ss_send[0]
    for k in range(ny - 1):
        total_squares = total_squares + ss_recv[k]
    scale = lax.rsqrt(as_column(total_squares[0:1, :], part) / DI + EPSILON)
    for copy in second[:2]:
        copy.wait_recv()
    for side in (0, 1):
        base = (1 - side) * half
        for c in range(0, half, 256):
            cols = slice(base + c, base + c + 256)
            own_ref[:, cols] = own_ref[:, cols] + r2_recv[side, 0, :, c : c + 256].astype(F32)
    for side in (0, 1):
        second[2 + side].wait_recv()
        base = side * half
        for c in range(0, half, 256):
            cols = slice(base + c, base + c + 256)
            value = own_ref[:, cols] + r2_recv[side, 1, :, c : c + 256].astype(F32)
            out_ref[:, cols] = (value * scale).astype(BF16)
    for copy in sends + squares_sent + first + second:
        copy.wait_send()


def local(nx, nr, ny, stream, gate, inc, outc, step_raw, bias, rate, skip, gain, proj, starts):
    tokens, channels = stream.shape
    heads = step_raw.shape[0]
    state = inc.shape[1]
    width = proj.shape[1]
    sr = state // nr
    part = tokens // ny
    anyspace = pl.BlockSpec(memory_space=pl.ANY)
    vmem = pl.BlockSpec(memory_space=pltpu.VMEM)
    dma = pltpu.SemaphoreType.DMA
    scratch = [
        pltpu.VMEM((tokens, channels), BF16),
        pltpu.VMEM((tokens, channels), BF16),
        pltpu.VMEM((tokens, state), BF16),
        pltpu.VMEM((tokens, state), BF16),
        pltpu.VMEM((heads, tokens), F32),
        pltpu.VMEM((channels, width), BF16),
        pltpu.VMEM((LANE, tokens + LANE), F32),
        pltpu.VMEM((tokens + LANE, LANE), BF16),
        pltpu.VMEM((LANE, channels), BF16),
        pltpu.VMEM((tokens, channels), BF16),
        pltpu.VMEM((128, tokens), BF16),
        pltpu.VMEM((tokens, state), BF16),
        pltpu.VMEM((tokens, channels), F32),
        pltpu.VMEM((tokens, channels), F32),
        pltpu.VMEM((24, channels), F32),
        pltpu.VMEM((nr, sr, channels + LANE), BF16),
        pltpu.VMEM((nr, sr, channels + LANE), BF16),
        pltpu.VMEM((16, LANE), F32),
        pltpu.VMEM((16, channels), F32),
        pltpu.VMEM((nr, sr, channels), F32),
        pltpu.VMEM((16, channels), F32),
        pltpu.VMEM((sr, channels + LANE), BF16),
        pltpu.VMEM((nx, sr, channels + LANE), BF16),
        pltpu.VMEM((nr, sr, channels), BF16),
        pltpu.VMEM((nr, sr, channels), BF16),
        pltpu.VMEM((state, channels), BF16),
        pltpu.VMEM((tokens, channels), BF16),
        pltpu.VMEM((2, part, width // 2), BF16),
        pltpu.VMEM((2, part, width // 2), BF16),
        pltpu.VMEM((2, 2, part, width // 2), BF16),
        pltpu.VMEM((2, 2, part, width // 2), BF16),
        pltpu.VMEM((part, width), F32),
        pltpu.VMEM((ny, 8, part), F32),
        pltpu.VMEM((ny - 1, 8, part), F32),
        dma((6,)),
        dma((nr - 1,)),
        dma((nr - 1,)),
        dma((nx - 1,)),
        dma((nx - 1,)),
        dma((nr - 1,)),
        dma((nr - 1,)),
        dma((2,)),
        dma((2,)),
        dma((2, 2)),
        dma((2, 2)),
        dma((ny - 1,)),
        dma((ny - 1,)),
    ]
    return pl.pallas_call(
        functools.partial(kernel, nx, nr, ny),
        out_shape=jax.ShapeDtypeStruct((part, width), BF16),
        in_specs=[anyspace] * 5 + [vmem] * 4 + [anyspace, vmem],
        out_specs=vmem,
        scratch_shapes=scratch,
        compiler_params=pltpu.CompilerParams(
            collective_id=0, has_side_effects=True, vmem_limit_bytes=56 * 1024 * 1024
        ),
        name="ssd_layer",
    )(
        stream,
        gate,
        inc,
        outc,
        step_raw,
        bias[None],
        rate[None],
        skip[None],
        gain[None],
        proj,
        starts[None],
    )


def solution(mesh):
    devices = mesh.shape["seq"]
    nr = min(ROW, devices // 2)
    in_specs = (
        P("seq", "head"),
        P("seq", "head"),
        P("seq", None),
        P("seq", None),
        P("head", "seq"),
        P("head"),
        P("head"),
        P("head"),
        P("head"),
        P("head", None),
        P(),
    )
    return jax.shard_map(
        functools.partial(local, devices // nr, nr, mesh.shape["head"]),
        mesh=mesh,
        in_specs=in_specs,
        out_specs=P(("seq", "head"), None),
        check_vma=False,
    )
```

```python
import functools

import jax
import jax.numpy as jnp
from jax import lax
from jax.experimental import pallas as pl
from jax.experimental.pallas import tpu as pltpu
from jax.sharding import PartitionSpec as P

DI = 5120
EPSILON = 1e-05
ALONG_Z = 8
LANE = 128
F32 = jnp.float32
BF16 = jnp.bfloat16
MESH = pl.DeviceIdType.MESH


def dot(a, b):
    return jnp.dot(a, b, preferred_element_type=F32)


def dot_nt(a, b):
    return lax.dot_general(a, b, (((1,), (1,)), ((), ())), preferred_element_type=F32)


def rounded(v):
    return v.astype(BF16).astype(F32)


def eye_mask(n):
    return lax.broadcasted_iota(jnp.int32, (n, n), 0) == lax.broadcasted_iota(jnp.int32, (n, n), 1)


def as_column(row, n):
    return jnp.sum(jnp.where(eye_mask(n), row, 0.0), axis=1, keepdims=True)


def as_row(column, n):
    return jnp.sum(jnp.where(eye_mask(n), column, 0.0), axis=0, keepdims=True)


def link_tile(row, rows):
    high = rounded(row)
    middle = rounded(row - high)
    low = row - high - middle
    at = lax.broadcasted_iota(jnp.int32, (rows, LANE), 0)
    return jnp.where(
        at == 0, high, jnp.where(at == 1, middle, jnp.where(at == 2, low, 0.0))
    ).astype(BF16)


def kernel(
    nx,
    nz,
    ny,
    x_hbm,
    g_hbm,
    b_hbm,
    c_hbm,
    st_hbm,
    bias_ref,
    rate_ref,
    skip_ref,
    gain_ref,
    w_hbm,
    doc_ref,
    out_hbm,
    x_v,
    g_v,
    b_v,
    c_v,
    st_v,
    w_v,
    m_ref,
    mt_ref,
    e_ref,
    v_ref,
    sc_ref,
    cj_ref,
    a1_ref,
    a2_ref,
    row_ref,
    own_s,
    pair_send,
    pair_recv,
    first_s,
    asend,
    arecv,
    ll_ref,
    lx_ref,
    l0_ref,
    pre_ref,
    pl_ref,
    xsend,
    xrecv,
    bsend,
    brecv,
    fsend,
    frecv,
    sp_ref,
    hid_ref,
    r1_send,
    r1_recv,
    r2_send,
    r2_recv,
    own_ref,
    out_v,
    ss_send,
    ss_recv,
    copy_sem,
    p_sem,
    a_ssem,
    a_rsem,
    x_ssem,
    x_rsem,
    b_ssem,
    b_rsem,
    f_ssem,
    f_rsem,
    r1_ssem,
    r1_rsem,
    r2_ssem,
    r2_rsem,
    ss_ssem,
    ss_rsem,
    out_sem,
):
    seq = lax.axis_index("seq")
    head = lax.axis_index("head")
    core = seq % 2
    z = (seq // 2) % nz
    xi = seq // (2 * nz)
    is_first = core == 0
    tokens, channels = x_v.shape
    heads = st_v.shape[0]
    state = b_v.shape[1]
    width = w_v.shape[1]
    half = width // 2
    side_width = channels // 2
    sr = state // nz
    part = tokens // ny
    offset = seq * tokens
    head_size = channels // heads

    loads = [
        pltpu.make_async_copy(src, dst, copy_sem.at[i])
        for i, (src, dst) in enumerate(
            (
                (st_hbm, st_v),
                (b_hbm, b_v),
                (x_hbm, x_v),
                (c_hbm, c_v),
                (g_hbm, g_v),
                (w_hbm, w_v),
            )
        )
    ]
    for load in loads[:3]:
        load.start()

    barrier = pltpu.get_barrier_semaphore()
    partner = (seq + 1 - 2 * core, head)
    in_z = [((xi * nz + (z + k) % nz) * 2 + core, head) for k in range(nz)]
    in_x = [((((xi + k) % nx) * nz + z) * 2 + core, head) for k in range(nx)]
    in_y = [(seq, (head + k) % ny) for k in range(ny)]
    greeted = in_z[1:] + in_x[1:] + in_y[1:] + [partner]
    for device in greeted:
        pl.semaphore_signal(barrier, inc=1, device_id=device, device_id_type=MESH)

    def send(src, dst, ssem, rsem, device):
        copy = pltpu.make_async_remote_copy(
            src_ref=src,
            dst_ref=dst,
            send_sem=ssem,
            recv_sem=rsem,
            device_id=device,
            device_id_type=MESH,
        )
        copy.start()
        return copy

    def around(n):
        order = []
        for d in range(n // 2, 0, -1):
            order += [d] if 2 * d == n else [d, n - d]
        return order

    e_ref[...] = (
        (lax.broadcasted_iota(jnp.int32, (LANE, channels), 0) & 31)
        == lax.broadcasted_iota(jnp.int32, (LANE, channels), 1) // head_size
    ).astype(F32).astype(BF16)
    m_ref[...] = jnp.zeros_like(m_ref)
    ll_ref[...] = jnp.zeros_like(ll_ref)
    starts = doc_ref[...]
    position = offset + lax.broadcasted_iota(jnp.int32, (tokens, 1), 0)
    doc_start = jnp.max(
        jnp.where(starts <= position, starts.astype(F32), -1.0), axis=1, keepdims=True
    )
    joined = doc_start < offset.astype(F32)
    last_start = doc_start[tokens - 1 :, :]

    bias = as_column(bias_ref[...], heads)
    rate = as_column(rate_ref[...], heads)
    skip = as_column(skip_ref[...], heads)
    loads[0].wait()
    step = st_v[...] + bias
    step = jnp.maximum(step, 0.0) + jnp.log1p(jnp.exp(-jnp.abs(step)))
    cum = -step * rate
    lane = lax.broadcasted_iota(jnp.int32, (heads, tokens), 1)
    shift = 1
    while shift < tokens:
        cum = cum + jnp.where(lane >= shift, pltpu.roll(cum, shift, 1), 0.0)
        shift *= 2
    mid = cum[:, tokens // 2 - 1 : tokens // 2]
    total = cum[:, tokens - 1 :]
    before_scale = jnp.exp(mid - cum) * step
    after_scale = jnp.exp(cum - mid)

    def put(first, columns, value):
        high = rounded(value)
        m_ref[first : first + heads, columns] = high
        m_ref[first + 32 : first + 32 + heads, columns] = value - high

    wide = (heads, LANE)
    put(0, slice(0, tokens), before_scale)
    put(64, slice(0, tokens), after_scale)
    put(0, slice(tokens, tokens + LANE), jnp.broadcast_to(jnp.exp(mid), wide))
    put(64, slice(tokens, tokens + LANE), jnp.broadcast_to(skip, wide))
    mt_ref[...] = m_ref[...].T.astype(BF16)
    gate_row = jnp.where(last_start < offset.astype(F32), total, -1e30)
    link_row = jnp.sum(
        jnp.where(
            lax.broadcasted_iota(jnp.int32, (heads, LANE), 0)
            == lax.broadcasted_iota(jnp.int32, (heads, LANE), 1),
            gate_row,
            0.0,
        ),
        axis=0,
        keepdims=True,
    )

    def expand(rows, upper):
        block = mt_ref[rows, :]
        at = lax.broadcasted_iota(jnp.int32, block.shape, 1)
        block = jnp.where((at >= 64) if upper else (at < 64), block.astype(F32), 0.0)
        return block.astype(BF16)

    row_ref[0:8, :] = dot(expand(slice(tokens - 8, tokens), True), e_ref[...])
    row_ref[8:16, :] = dot(expand(slice(tokens, tokens + 8), False), e_ref[...])
    row_ref[16:24, :] = dot(expand(slice(tokens, tokens + 8), True), e_ref[...])

    step_rows = 128
    columns = [slice(c, c + 256) for c in range(0, channels, 256)]
    cuts = [(c, min(256, side_width - c)) for c in range(0, side_width, 256)]
    mine = core * side_width
    others = (1 - core) * side_width

    def lanes(base, cut):
        return pl.ds(pl.multiple_of(base + cut[0], LANE), cut[1])

    loads[1].wait()
    kept = jnp.where(position.astype(F32) >= last_start, b_v[...].astype(F32), 0.0)
    kept = kept.T.astype(BF16)
    loads[2].wait()
    for load in loads[3:]:
        load.start()

    def summary(base, store):
        @pl.loop(0, tokens // step_rows)
        def _(i):
            rows = pl.ds(pl.multiple_of(i * step_rows, step_rows), step_rows)
            left = expand(rows, False)
            for cut in cuts:
                cols = lanes(base, cut)
                v_ref[rows, cols] = (
                    x_v[rows, cols].astype(F32) * dot(left, e_ref[:, cols])
                ).astype(BF16)

        for cut in cuts:
            cols = lanes(base, cut)
            store(
                slice(cut[0], cut[0] + cut[1]),
                dot(kept, v_ref[:, cols]) * row_ref[7:8, cols],
            )

    def to_partner(cols, value):
        pair_send[0:state, cols] = value.astype(BF16)

    def to_own(cols, value):
        own_s[:, cols] = value

    pair_send[state:, :] = jnp.zeros((8, side_width), BF16)
    pair_send[state:, 0:LANE] = link_tile(link_row, 8)
    summary(others, to_partner)
    pl.semaphore_wait(barrier, len(greeted))
    pair = send(pair_send, pair_recv, p_sem.at[0], p_sem.at[1], partner)
    summary(mine, to_own)

    def link_of(block):
        return jnp.sum(block.astype(F32), axis=0, keepdims=True)

    def spread(logs):
        at = lax.broadcasted_iota(jnp.int32, logs.shape, 1)
        value = jnp.where(at < heads, jnp.exp(logs), 0.0)
        high = value.astype(BF16)
        rest = value - high.astype(F32)
        middle = rest.astype(BF16)
        low = (rest - middle.astype(F32)).astype(BF16)
        hot = e_ref[:, pl.ds(pl.multiple_of(mine, LANE), side_width)]
        return dot(high, hot) + dot(middle, hot) + dot(low, hot)

    pair.wait_recv()
    partner_row = link_of(pair_recv[state:, 0:LANE])
    ll_ref[0:1, :] = jnp.where(is_first, link_row, partner_row)
    ll_ref[1:2, :] = jnp.where(is_first, partner_row, link_row)
    chip_log = link_row + partner_row
    pair_links = spread(ll_ref[0:8, :])
    l0_ref[...] = pair_links[0:1, :]
    tile = link_tile(chip_log, sr)
    for j in range(nz):
        rows = slice(j * sr, (j + 1) * sr)
        own = own_s[rows, :]
        came = pair_recv[rows, :].astype(F32)
        earlier_core = jnp.where(is_first, own, came)
        first_s[rows, :] = earlier_core
        asend[j, :, 0:side_width] = (
            pair_links[1:2, :] * earlier_core + jnp.where(is_first, came, own)
        ).astype(BF16)
        asend[j, :, side_width:] = tile
    sends = [pair]
    row_copies = {}
    for k in around(nz):
        row_copies[k] = send(
            asend.at[(z + k) % nz],
            arecv.at[z],
            a_ssem.at[k - 1],
            a_rsem.at[k - 1],
            in_z[k],
        )
    arecv[z] = asend[z]

    loads[3].wait()
    cj_ref[...] = jnp.where(joined, c_v[...].astype(F32), 0.0).astype(BF16)
    loads[4].wait()

    def alone(first):
        rows = pl.ds(first, step_rows)
        scores = dot_nt(c_v[rows, :], b_v[...])
        at = offset + first + lax.broadcasted_iota(jnp.int32, (step_rows, 1), 0)
        source = offset + lax.broadcasted_iota(jnp.int32, (step_rows, tokens), 1)
        begun = jnp.max(
            jnp.where(starts <= at, starts.astype(F32), -1.0), axis=1, keepdims=True
        )
        live = (source <= at) & (source.astype(F32) >= begun)
        sc_ref[...] = jnp.where(live, scores, 0.0).astype(BF16)
        left = expand(rows, True)
        for cols in columns:
            scale = dot(left, e_ref[:, cols])
            gate = g_v[rows, cols].astype(F32)
            gate = gate / (1.0 + jnp.exp(-gate))
            inside = dot(sc_ref[...], v_ref[:, cols])
            skipped = row_ref[16:17, cols] * x_v[rows, cols].astype(F32)
            a1_ref[rows, cols] = scale * gate
            a2_ref[rows, cols] = (scale * inside + skipped) * gate

    @pl.loop(0, tokens // step_rows)
    def _(i):
        alone(pl.multiple_of(i * step_rows, step_rows))

    for k in around(nz):
        row_copies[k].wait_recv()
    for j in range(nz):
        ll_ref[j : j + 1, :] = link_of(arecv[j, :, side_width:])
    row_log = jnp.sum(ll_ref[0:nz, :], axis=0, keepdims=True)
    lx_ref[0:nz, :] = spread(ll_ref[0:nz, :])
    prefix = jnp.zeros((sr, side_width), F32)
    product = jnp.ones((1, side_width), F32)
    for j in range(nz):
        pre_ref[j] = prefix
        pl_ref[j : j + 1, :] = product
        link = lx_ref[j : j + 1, :]
        prefix = link * prefix + arecv[j, :, 0:side_width].astype(F32)
        product = product * link
    xsend[:, 0:side_width] = prefix.astype(BF16)
    xsend[:, side_width:] = link_tile(row_log, sr)
    x_copies = {}
    for k in around(nx):
        x_copies[k] = send(
            xsend, xrecv.at[xi], x_ssem.at[k - 1], x_rsem.at[k - 1], in_x[k]
        )
    xrecv[xi] = xsend[...]
    for k in around(nx):
        x_copies[k].wait_recv()
    for j in range(nx):
        ll_ref[j : j + 1, :] = link_of(xrecv[j, :, side_width:])
    lx_ref[0:nx, :] = spread(ll_ref[0:nx, :])
    earlier = jnp.zeros((sr, side_width), F32)
    for j in range(nx - 1):
        after = lx_ref[j : j + 1, :] * earlier + xrecv[j, :, 0:side_width].astype(F32)
        earlier = jnp.where(j < xi, after, earlier)
    for j in range(nz):
        bsend[j] = (pre_ref[j] + pl_ref[j : j + 1, :] * earlier).astype(BF16)
    back_copies = {}
    for k in around(nz):
        back_copies[k] = send(
            bsend.at[(z + k) % nz],
            brecv.at[z],
            b_ssem.at[k - 1],
            b_rsem.at[k - 1],
            in_z[k],
        )
    brecv[z] = bsend[z]

    own_lanes = pl.ds(pl.multiple_of(mine, LANE), side_width)
    other_lanes = pl.ds(pl.multiple_of(others, LANE), side_width)
    final_copies = []
    for k in [0] + around(nz)[::-1]:
        if k:
            back_copies[k].wait_recv()
        slot = (z + nz - k) % nz
        rows = pl.ds(pl.multiple_of(slot * sr, sr), sr)
        to_first = brecv[slot].astype(F32)
        to_second = l0_ref[...] * to_first + first_s[rows, :]
        fsend[slot] = jnp.where(is_first, to_second, to_first).astype(BF16)
        final_copies.append(
            send(fsend.at[slot], frecv.at[slot], f_ssem.at[k], f_rsem.at[k], partner)
        )
        sp_ref[rows, own_lanes] = (
            row_ref[8:9, own_lanes] * jnp.where(is_first, to_first, to_second)
        ).astype(BF16)

    sends += [*row_copies.values(), *x_copies.values(), *back_copies.values(), *final_copies]

    def chunk_rows(k):
        return pl.ds(pl.multiple_of(((head + k) % ny) * part, part), part)

    def hidden_columns(rows, cols):
        gated = a2_ref[rows, cols] + a1_ref[rows, cols] * dot(cj_ref[rows, :], sp_ref[:, cols])
        hid_ref[rows, cols] = (gated * gain_ref[cols].reshape(1, cols.size)).astype(BF16)
        return jnp.sum(gated * gated, axis=1, keepdims=True)

    def share_squares(k, squares):
        ss_send[k] = jnp.broadcast_to(as_row(squares, part), (8, part))
        if k:
            return send(
                ss_send.at[k],
                ss_recv.at[k - 1],
                ss_ssem.at[k - 1],
                ss_rsem.at[k - 1],
                in_y[k],
            )

    def make_hidden(k):
        rows = chunk_rows(k)
        squares = jnp.zeros((part, 1), F32)
        for cols in columns:
            squares = squares + hidden_columns(rows, pl.ds(cols.start, 256))
        return share_squares(k, squares)

    def project(k, base, span, store):
        rows = chunk_rows(k)
        for c in range(span[0], span[1], 256):
            store(
                slice(c, c + 256),
                dot(hid_ref[rows, :], w_v[:, base + c : base + c + 256]),
            )

    def into(ref):
        def store(cols, value):
            ref[:, cols] = value.astype(BF16)

        return store

    def added(ref, extra):
        def store(cols, value):
            ref[:, cols] = (value + extra[:, cols].astype(F32)).astype(BF16)

        return store

    far = chunk_rows(2)
    squares = jnp.zeros((part, 1), F32)
    for cut in cuts:
        squares = squares + hidden_columns(far, lanes(mine, cut))
    for copy in final_copies:
        copy.wait_recv()
    for j in range(nz):
        rows = slice(j * sr, (j + 1) * sr)
        sp_ref[rows, other_lanes] = (row_ref[8:9, other_lanes] * frecv[j].astype(F32)).astype(
            BF16
        )
    for cut in cuts:
        squares = squares + hidden_columns(far, lanes(others, cut))
    loads[5].wait()
    up, down = in_y[1], in_y[ny - 1]
    spans = ((0, 512), (512, half))
    first = {}
    for p, span in enumerate(spans):
        for side, device in ((0, up), (1, down)):
            project(2, side * half, span, into(r1_send.at[side]))
            cols = slice(*span)
            first[side, p] = send(
                r1_send.at[side, :, cols],
                r1_recv.at[side, :, cols],
                r1_ssem.at[side, p],
                r1_rsem.at[side, p],
                device,
            )
    squares_sent = [share_squares(2, squares)]
    second = {}
    for side, k, device in ((0, 1, up), (1, ny - 1, down)):
        squares_sent.append(make_hidden(k))
        project(k, (1 - side) * half, (0, half), into(r2_send.at[side, 0]))
        second[side, 0] = send(
            r2_send.at[side, 0],
            r2_recv.at[side, 0],
            r2_ssem.at[side, 0],
            r2_rsem.at[side, 0],
            device,
        )
    make_hidden(0)
    for side in (0, 1):

        def store(cols, value, side=side):
            own_ref[:, side * half + cols.start : side * half + cols.stop] = value

        project(0, side * half, (0, half), store)
    for p, span in enumerate(spans):
        for side, k, device in ((0, 1, up), (1, ny - 1, down)):
            first[side, p].wait_recv()
            project(k, side * half, span, added(r2_send.at[side, 1], r1_recv.at[side]))
            cols = slice(*span)
            second[side, 1 + p] = send(
                r2_send.at[side, 1, :, cols],
                r2_recv.at[side, 1, :, cols],
                r2_ssem.at[side, 1 + p],
                r2_rsem.at[side, 1 + p],
                device,
            )
    for copy in squares_sent:
        copy.wait_recv()
    total_squares = ss_send[0]
    for k in range(ny - 1):
        total_squares = total_squares + ss_recv[k]
    scale = lax.rsqrt(as_column(total_squares[0:1, :], part) / DI + EPSILON)
    for side in (0, 1):
        second[side, 0].wait_recv()
        base = (1 - side) * half
        for c in range(0, half, 256):
            cols = slice(base + c, base + c + 256)
            own_ref[:, cols] = own_ref[:, cols] + r2_recv[side, 0, :, c : c + 256].astype(F32)
    leaving = []
    for p, span in enumerate(spans):
        for side in (0, 1):
            second[side, 1 + p].wait_recv()
            base = side * half
            for c in range(span[0], span[1], 256):
                cols = slice(base + c, base + c + 256)
                value = own_ref[:, cols] + r2_recv[side, 1, :, c : c + 256].astype(F32)
                out_v[:, cols] = (value * scale).astype(BF16)
            cols = slice(base + span[0], base + span[1])
            copy = pltpu.make_async_copy(
                out_v.at[:, cols], out_hbm.at[:, cols], out_sem.at[side, p]
            )
            copy.start()
            leaving.append(copy)
    for copy in sends + squares_sent + [*first.values(), *second.values()]:
        copy.wait_send()
    for copy in leaving:
        copy.wait()


def local(nx, nz, ny, stream, gate, inc, outc, step_raw, bias, rate, skip, gain, proj, starts):
    tokens, channels = stream.shape
    heads = step_raw.shape[0]
    state = inc.shape[1]
    width = proj.shape[1]
    half = width // 2
    sw = channels // 2
    sr = state // nz
    part = tokens // ny
    anyspace = pl.BlockSpec(memory_space=pl.ANY)
    vmem = pl.BlockSpec(memory_space=pltpu.VMEM)
    dma = pltpu.SemaphoreType.DMA
    scratch = [
        pltpu.VMEM((tokens, channels), BF16),
        pltpu.VMEM((tokens, channels), BF16),
        pltpu.VMEM((tokens, state), BF16),
        pltpu.VMEM((tokens, state), BF16),
        pltpu.VMEM((heads, tokens), F32),
        pltpu.VMEM((channels, width), BF16),
        pltpu.VMEM((LANE, tokens + LANE), F32),
        pltpu.VMEM((tokens + LANE, LANE), BF16),
        pltpu.VMEM((LANE, channels), BF16),
        pltpu.VMEM((tokens, channels), BF16),
        pltpu.VMEM((128, tokens), BF16),
        pltpu.VMEM((tokens, state), BF16),
        pltpu.VMEM((tokens, channels), F32),
        pltpu.VMEM((tokens, channels), F32),
        pltpu.VMEM((24, channels), F32),
        pltpu.VMEM((state, sw), F32),
        pltpu.VMEM((state + 8, sw), BF16),
        pltpu.VMEM((state + 8, sw), BF16),
        pltpu.VMEM((state, sw), F32),
        pltpu.VMEM((nz, sr, sw + LANE), BF16),
        pltpu.VMEM((nz, sr, sw + LANE), BF16),
        pltpu.VMEM((8, LANE), F32),
        pltpu.VMEM((8, sw), F32),
        pltpu.VMEM((1, sw), F32),
        pltpu.VMEM((nz, sr, sw), F32),
        pltpu.VMEM((8, sw), F32),
        pltpu.VMEM((sr, sw + LANE), BF16),
        pltpu.VMEM((nx, sr, sw + LANE), BF16),
        pltpu.VMEM((nz, sr, sw), BF16),
        pltpu.VMEM((nz, sr, sw), BF16),
        pltpu.VMEM((nz, sr, sw), BF16),
        pltpu.VMEM((nz, sr, sw), BF16),
        pltpu.VMEM((state, channels), BF16),
        pltpu.VMEM((tokens, channels), BF16),
        pltpu.VMEM((2, part, half), BF16),
        pltpu.VMEM((2, part, half), BF16),
        pltpu.VMEM((2, 2, part, half), BF16),
        pltpu.VMEM((2, 2, part, half), BF16),
        pltpu.VMEM((part, width), F32),
        pltpu.VMEM((part, width), BF16),
        pltpu.VMEM((ny, 8, part), F32),
        pltpu.VMEM((ny - 1, 8, part), F32),
        dma((6,)),
        dma((2,)),
        dma((nz - 1,)),
        dma((nz - 1,)),
        dma((nx - 1,)),
        dma((nx - 1,)),
        dma((nz - 1,)),
        dma((nz - 1,)),
        dma((nz,)),
        dma((nz,)),
        dma((2, 2)),
        dma((2, 2)),
        dma((2, 3)),
        dma((2, 3)),
        dma((ny - 1,)),
        dma((ny - 1,)),
        dma((2, 2)),
    ]
    return pl.pallas_call(
        functools.partial(kernel, nx, nz, ny),
        out_shape=jax.ShapeDtypeStruct((part, width), BF16),
        in_specs=[anyspace] * 5 + [vmem] * 4 + [anyspace, vmem],
        out_specs=anyspace,
        scratch_shapes=scratch,
        compiler_params=pltpu.CompilerParams(
            collective_id=0, has_side_effects=True, vmem_limit_bytes=56 * 1024 * 1024
        ),
        name="ssd_layer",
    )(
        stream,
        gate,
        inc,
        outc,
        step_raw,
        bias[None],
        rate[None],
        skip[None],
        gain,
        proj,
        starts[None],
    )


def solution(mesh):
    chips = mesh.shape["seq"] // 2
    nz = min(ALONG_Z, chips)
    in_specs = (
        P("seq", "head"),
        P("seq", "head"),
        P("seq", None),
        P("seq", None),
        P("head", "seq"),
        P("head"),
        P("head"),
        P("head"),
        P("head"),
        P("head", None),
        P(),
    )
    return jax.shard_map(
        functools.partial(local, chips // nz, nz, mesh.shape["head"]),
        mesh=mesh,
        in_specs=in_specs,
        out_specs=P(("seq", "head"), None),
        check_vma=False,
    )
```

```python
import functools

import jax
import jax.numpy as jnp
from jax import lax
from jax.experimental import pallas as pl
from jax.experimental.pallas import tpu as pltpu
from jax.sharding import PartitionSpec as P

DI = 5120
EPSILON = 1e-05
ALONG_Z = 8
LANE = 128
F32 = jnp.float32
BF16 = jnp.bfloat16
MESH = pl.DeviceIdType.MESH


def dot(a, b):
    return jnp.dot(a, b, preferred_element_type=F32)


def dot_nt(a, b):
    return lax.dot_general(a, b, (((1,), (1,)), ((), ())), preferred_element_type=F32)


def rounded(v):
    return v.astype(BF16).astype(F32)


def eye_mask(n):
    return lax.broadcasted_iota(jnp.int32, (n, n), 0) == lax.broadcasted_iota(jnp.int32, (n, n), 1)


def as_column(row, n):
    return jnp.sum(jnp.where(eye_mask(n), row, 0.0), axis=1, keepdims=True)


def as_row(column, n):
    return jnp.sum(jnp.where(eye_mask(n), column, 0.0), axis=0, keepdims=True)


def link_tile(row, rows):
    high = rounded(row)
    middle = rounded(row - high)
    low = row - high - middle
    at = lax.broadcasted_iota(jnp.int32, (rows, LANE), 0)
    return jnp.where(
        at == 0, high, jnp.where(at == 1, middle, jnp.where(at == 2, low, 0.0))
    ).astype(BF16)


def kernel(
    nx,
    nz,
    ny,
    x_hbm,
    g_hbm,
    b_hbm,
    c_hbm,
    st_hbm,
    bias_hbm,
    rate_hbm,
    skip_hbm,
    gain_hbm,
    w_hbm,
    doc_hbm,
    out_hbm,
    bias_ref,
    rate_ref,
    skip_ref,
    gain_ref,
    doc_ref,
    x_v,
    g_v,
    b_v,
    c_v,
    st_v,
    w_v,
    m_ref,
    mt_ref,
    e_ref,
    v_ref,
    sc_ref,
    cj_ref,
    a1_ref,
    a2_ref,
    row_ref,
    own_s,
    pair_send,
    pair_recv,
    first_s,
    asend,
    arecv,
    zlog_send,
    zlog_recv,
    xlog_send,
    xlog_recv,
    ll_ref,
    lx_ref,
    l0_ref,
    pre_ref,
    pl_ref,
    xsend,
    xrecv,
    bsend,
    brecv,
    fsend,
    frecv,
    sp_ref,
    hid_ref,
    r1_send,
    r1_recv,
    r2_send,
    r2_recv,
    own_ref,
    out_v,
    ss_send,
    ss_recv,
    small_sem,
    copy_sem,
    p_sem,
    la_ssem,
    la_rsem,
    lx_ssem,
    lx_rsem,
    a_ssem,
    a_rsem,
    x_ssem,
    x_rsem,
    b_ssem,
    b_rsem,
    f_ssem,
    f_rsem,
    r1_ssem,
    r1_rsem,
    r2_ssem,
    r2_rsem,
    ss_ssem,
    ss_rsem,
    out_sem,
):
    seq = lax.axis_index("seq")
    head = lax.axis_index("head")
    core = seq % 2
    z = (seq // 2) % nz
    xi = seq // (2 * nz)
    is_first = core == 0
    tokens, channels = x_v.shape
    heads = st_v.shape[0]
    state = b_v.shape[1]
    width = w_v.shape[1]
    half = width // 2
    side_width = channels // 2
    sr = state // nz
    part = tokens // ny
    offset = seq * tokens
    head_size = channels // heads

    barrier = pltpu.get_barrier_semaphore()
    partner = (seq + 1 - 2 * core, head)
    in_z = [((xi * nz + (z + k) % nz) * 2 + core, head) for k in range(nz)]
    in_x = [((((xi + k) % nx) * nz + z) * 2 + core, head) for k in range(nx)]
    in_y = [(seq, (head + k) % ny) for k in range(ny)]
    greeted = in_z[1:] + in_x[1:] + in_y[1:] + [partner]
    for device in greeted:
        pl.semaphore_signal(barrier, inc=1, device_id=device, device_id_type=MESH)

    small = [
        pltpu.make_async_copy(src, dst, small_sem.at[i])
        for i, (src, dst) in enumerate(
            (
                (doc_hbm, doc_ref),
                (bias_hbm, bias_ref),
                (rate_hbm, rate_ref),
                (skip_hbm, skip_ref),
                (gain_hbm, gain_ref),
            )
        )
    ]
    loads = [
        pltpu.make_async_copy(src, dst, copy_sem.at[i])
        for i, (src, dst) in enumerate(
            (
                (st_hbm, st_v),
                (b_hbm, b_v),
                (x_hbm, x_v),
                (c_hbm, c_v),
                (g_hbm, g_v),
                (w_hbm, w_v),
            )
        )
    ]
    for load in [loads[0], *small, *loads[1:3]]:
        load.start()

    def send(src, dst, ssem, rsem, device):
        copy = pltpu.make_async_remote_copy(
            src_ref=src,
            dst_ref=dst,
            send_sem=ssem,
            recv_sem=rsem,
            device_id=device,
            device_id_type=MESH,
        )
        copy.start()
        return copy

    def around(n):
        order = []
        for d in range(n // 2, 0, -1):
            order += [d] if 2 * d == n else [d, n - d]
        return order

    e_ref[...] = (
        (lax.broadcasted_iota(jnp.int32, (LANE, channels), 0) & 31)
        == lax.broadcasted_iota(jnp.int32, (LANE, channels), 1) // head_size
    ).astype(F32).astype(BF16)
    m_ref[...] = jnp.zeros_like(m_ref)
    ll_ref[...] = jnp.zeros_like(ll_ref)
    small[0].wait()
    starts = doc_ref[...]
    position = offset + lax.broadcasted_iota(jnp.int32, (tokens, 1), 0)
    doc_start = jnp.max(
        jnp.where(starts <= position, starts.astype(F32), -1.0), axis=1, keepdims=True
    )
    joined = doc_start < offset.astype(F32)
    last_start = doc_start[tokens - 1 :, :]

    for load in small[1:]:
        load.wait()
    bias = as_column(bias_ref[...], heads)
    rate = as_column(rate_ref[...], heads)
    skip = as_column(skip_ref[...], heads)
    loads[0].wait()
    step = st_v[...] + bias
    step = jnp.maximum(step, 0.0) + jnp.log1p(jnp.exp(-jnp.abs(step)))
    cum = -step * rate
    lane = lax.broadcasted_iota(jnp.int32, (heads, tokens), 1)
    shift = 1
    while shift < tokens:
        cum = cum + jnp.where(lane >= shift, pltpu.roll(cum, shift, 1), 0.0)
        shift *= 2
    mid = cum[:, tokens // 2 - 1 : tokens // 2]
    total = cum[:, tokens - 1 :]
    before_scale = jnp.exp(mid - cum) * step
    after_scale = jnp.exp(cum - mid)

    def put(first, columns, value):
        high = rounded(value)
        m_ref[first : first + heads, columns] = high
        m_ref[first + 32 : first + 32 + heads, columns] = value - high

    wide = (heads, LANE)
    put(0, slice(0, tokens), before_scale)
    put(64, slice(0, tokens), after_scale)
    put(0, slice(tokens, tokens + LANE), jnp.broadcast_to(jnp.exp(mid), wide))
    put(64, slice(tokens, tokens + LANE), jnp.broadcast_to(skip, wide))
    mt_ref[...] = m_ref[...].T.astype(BF16)
    gate_row = jnp.where(last_start < offset.astype(F32), total, -1e30)
    link_row = jnp.sum(
        jnp.where(
            lax.broadcasted_iota(jnp.int32, (heads, LANE), 0)
            == lax.broadcasted_iota(jnp.int32, (heads, LANE), 1),
            gate_row,
            0.0,
        ),
        axis=0,
        keepdims=True,
    )

    def expand(rows, upper):
        block = mt_ref[rows, :]
        at = lax.broadcasted_iota(jnp.int32, block.shape, 1)
        block = jnp.where((at >= 64) if upper else (at < 64), block.astype(F32), 0.0)
        return block.astype(BF16)

    row_ref[0:8, :] = dot(expand(slice(tokens - 8, tokens), True), e_ref[...])
    row_ref[8:16, :] = dot(expand(slice(tokens, tokens + 8), False), e_ref[...])
    row_ref[16:24, :] = dot(expand(slice(tokens, tokens + 8), True), e_ref[...])

    step_rows = 128
    columns = [slice(c, c + 256) for c in range(0, channels, 256)]
    cuts = [(c, min(256, side_width - c)) for c in range(0, side_width, 256)]
    mine = core * side_width
    others = (1 - core) * side_width

    def lanes(base, cut):
        return pl.ds(pl.multiple_of(base + cut[0], LANE), cut[1])

    loads[1].wait()
    kept = jnp.where(position.astype(F32) >= last_start, b_v[...].astype(F32), 0.0)
    kept = kept.T.astype(BF16)
    loads[2].wait()
    for load in loads[3:]:
        load.start()

    def summary(base, store):
        @pl.loop(0, tokens // step_rows)
        def _(i):
            rows = pl.ds(pl.multiple_of(i * step_rows, step_rows), step_rows)
            left = expand(rows, False)
            for cut in cuts:
                cols = lanes(base, cut)
                v_ref[rows, cols] = (
                    x_v[rows, cols].astype(F32) * dot(left, e_ref[:, cols])
                ).astype(BF16)

        for cut in cuts:
            cols = lanes(base, cut)
            store(
                slice(cut[0], cut[0] + cut[1]),
                dot(kept, v_ref[:, cols]) * row_ref[7:8, cols],
            )

    def to_partner(cols, value):
        pair_send[0:state, cols] = value.astype(BF16)

    def to_own(cols, value):
        own_s[:, cols] = value

    pair_send[state:, :] = jnp.zeros((8, side_width), BF16)
    pair_send[state:, 0:LANE] = link_tile(link_row, 8)
    summary(others, to_partner)
    pl.semaphore_wait(barrier, len(greeted))
    pair = send(pair_send, pair_recv, p_sem.at[0], p_sem.at[1], partner)
    summary(mine, to_own)

    def link_of(block):
        return jnp.sum(block.astype(F32), axis=0, keepdims=True)

    def spread(logs):
        at = lax.broadcasted_iota(jnp.int32, logs.shape, 1)
        value = jnp.where(at < heads, jnp.exp(logs), 0.0)
        high = value.astype(BF16)
        rest = value - high.astype(F32)
        middle = rest.astype(BF16)
        low = (rest - middle.astype(F32)).astype(BF16)
        hot = e_ref[:, pl.ds(pl.multiple_of(mine, LANE), side_width)]
        return dot(high, hot) + dot(middle, hot) + dot(low, hot)

    pair.wait_recv()
    partner_row = link_of(pair_recv[state:, 0:LANE])
    ll_ref[0:1, :] = jnp.where(is_first, link_row, partner_row)
    ll_ref[1:2, :] = jnp.where(is_first, partner_row, link_row)
    chip_log = link_row + partner_row
    pair_links = spread(ll_ref[0:8, :])
    l0_ref[...] = pair_links[0:1, :]
    sends = [pair]
    zlog_send[...] = chip_log
    zlog_copies = {}
    for k in around(nz):
        zlog_copies[k] = send(
            zlog_send, zlog_recv.at[z], la_ssem.at[k - 1], la_rsem.at[k - 1], in_z[k]
        )
    zlog_recv[z] = chip_log
    for j in range(nz):
        rows = slice(j * sr, (j + 1) * sr)
        own = own_s[rows, :]
        came = pair_recv[rows, :].astype(F32)
        earlier_core = jnp.where(is_first, own, came)
        first_s[rows, :] = earlier_core
        asend[j] = (
            pair_links[1:2, :] * earlier_core + jnp.where(is_first, came, own)
        ).astype(BF16)
    row_copies = {}
    for k in around(nz):
        row_copies[k] = send(
            asend.at[(z + k) % nz],
            arecv.at[z],
            a_ssem.at[k - 1],
            a_rsem.at[k - 1],
            in_z[k],
        )
    arecv[z] = asend[z]

    loads[3].wait()
    cj_ref[...] = jnp.where(joined, c_v[...].astype(F32), 0.0).astype(BF16)
    loads[4].wait()

    def alone(first):
        rows = pl.ds(first, step_rows)
        scores = dot_nt(c_v[rows, :], b_v[...])
        at = offset + first + lax.broadcasted_iota(jnp.int32, (step_rows, 1), 0)
        source = offset + lax.broadcasted_iota(jnp.int32, (step_rows, tokens), 1)
        begun = jnp.max(
            jnp.where(starts <= at, starts.astype(F32), -1.0), axis=1, keepdims=True
        )
        live = (source <= at) & (source.astype(F32) >= begun)
        sc_ref[...] = jnp.where(live, scores, 0.0).astype(BF16)
        left = expand(rows, True)
        for cols in columns:
            scale = dot(left, e_ref[:, cols])
            gate = g_v[rows, cols].astype(F32)
            gate = gate / (1.0 + jnp.exp(-gate))
            inside = dot(sc_ref[...], v_ref[:, cols])
            skipped = row_ref[16:17, cols] * x_v[rows, cols].astype(F32)
            a1_ref[rows, cols] = scale * gate
            a2_ref[rows, cols] = (scale * inside + skipped) * gate

    @pl.loop(0, tokens // step_rows)
    def _(i):
        alone(pl.multiple_of(i * step_rows, step_rows))

    for k in around(nz):
        zlog_copies[k].wait_recv()
    for j in range(nz):
        ll_ref[j : j + 1, :] = zlog_recv[j]
    row_log = jnp.sum(ll_ref[0:nz, :], axis=0, keepdims=True)
    xlog_send[...] = row_log
    xlog_copies = {}
    for k in around(nx):
        xlog_copies[k] = send(
            xlog_send, xlog_recv.at[xi], lx_ssem.at[k - 1], lx_rsem.at[k - 1], in_x[k]
        )
    xlog_recv[xi] = row_log
    lx_ref[0:nz, :] = spread(ll_ref[0:nz, :])
    for k in around(nz):
        row_copies[k].wait_recv()
    prefix = jnp.zeros((sr, side_width), F32)
    product = jnp.ones((1, side_width), F32)
    for j in range(nz):
        pre_ref[j] = prefix
        pl_ref[j : j + 1, :] = product
        link = lx_ref[j : j + 1, :]
        prefix = link * prefix + arecv[j].astype(F32)
        product = product * link
    xsend[...] = prefix.astype(BF16)
    x_copies = {}
    for k in around(nx):
        x_copies[k] = send(
            xsend, xrecv.at[xi], x_ssem.at[k - 1], x_rsem.at[k - 1], in_x[k]
        )
    xrecv[xi] = xsend[...]
    for k in around(nx):
        xlog_copies[k].wait_recv()
    for j in range(nx):
        ll_ref[j : j + 1, :] = xlog_recv[j]
    lx_ref[0:nx, :] = spread(ll_ref[0:nx, :])
    for k in around(nx):
        x_copies[k].wait_recv()
    earlier = jnp.zeros((sr, side_width), F32)
    for j in range(nx - 1):
        after = lx_ref[j : j + 1, :] * earlier + xrecv[j].astype(F32)
        earlier = jnp.where(j < xi, after, earlier)
    for j in range(nz):
        bsend[j] = (pre_ref[j] + pl_ref[j : j + 1, :] * earlier).astype(BF16)
    back_copies = {}
    for k in around(nz):
        back_copies[k] = send(
            bsend.at[(z + k) % nz],
            brecv.at[z],
            b_ssem.at[k - 1],
            b_rsem.at[k - 1],
            in_z[k],
        )
    brecv[z] = bsend[z]

    own_lanes = pl.ds(pl.multiple_of(mine, LANE), side_width)
    other_lanes = pl.ds(pl.multiple_of(others, LANE), side_width)
    final_copies = []
    for k in [0] + around(nz)[::-1]:
        if k:
            back_copies[k].wait_recv()
        slot = (z + nz - k) % nz
        rows = pl.ds(pl.multiple_of(slot * sr, sr), sr)
        to_first = brecv[slot].astype(F32)
        to_second = l0_ref[...] * to_first + first_s[rows, :]
        fsend[slot] = jnp.where(is_first, to_second, to_first).astype(BF16)
        final_copies.append(
            send(fsend.at[slot], frecv.at[slot], f_ssem.at[k], f_rsem.at[k], partner)
        )
        sp_ref[rows, own_lanes] = (
            row_ref[8:9, own_lanes] * jnp.where(is_first, to_first, to_second)
        ).astype(BF16)

    for copies in (zlog_copies, row_copies, xlog_copies, x_copies, back_copies):
        sends += copies.values()
    sends += final_copies

    def chunk_rows(k):
        return pl.ds(pl.multiple_of(((head + k) % ny) * part, part), part)

    def hidden_columns(rows, cols):
        gated = a2_ref[rows, cols] + a1_ref[rows, cols] * dot(cj_ref[rows, :], sp_ref[:, cols])
        hid_ref[rows, cols] = (gated * gain_ref[cols].reshape(1, cols.size)).astype(BF16)
        return jnp.sum(gated * gated, axis=1, keepdims=True)

    def share_squares(k, squares):
        ss_send[k] = jnp.broadcast_to(as_row(squares, part), (8, part))
        if k:
            return send(
                ss_send.at[k],
                ss_recv.at[k - 1],
                ss_ssem.at[k - 1],
                ss_rsem.at[k - 1],
                in_y[k],
            )

    def make_hidden(k):
        rows = chunk_rows(k)
        squares = jnp.zeros((part, 1), F32)
        for cols in columns:
            squares = squares + hidden_columns(rows, pl.ds(cols.start, 256))
        return share_squares(k, squares)

    def project(k, base, span, store):
        rows = chunk_rows(k)
        for c in range(span[0], span[1], 256):
            store(
                slice(c, c + 256),
                dot(hid_ref[rows, :], w_v[:, base + c : base + c + 256]),
            )

    def into(ref):
        def store(cols, value):
            ref[:, cols] = value.astype(BF16)

        return store

    def added(ref, extra):
        def store(cols, value):
            ref[:, cols] = (value + extra[:, cols].astype(F32)).astype(BF16)

        return store

    far = chunk_rows(2)
    squares = jnp.zeros((part, 1), F32)
    for cut in cuts:
        squares = squares + hidden_columns(far, lanes(mine, cut))
    for copy in final_copies:
        copy.wait_recv()
    for j in range(nz):
        rows = slice(j * sr, (j + 1) * sr)
        sp_ref[rows, other_lanes] = (row_ref[8:9, other_lanes] * frecv[j].astype(F32)).astype(
            BF16
        )
    for cut in cuts:
        squares = squares + hidden_columns(far, lanes(others, cut))
    loads[5].wait()
    up, down = in_y[1], in_y[ny - 1]
    spans = ((0, 256), (256, half))
    last_spans = ((0, half - 256), (half - 256, half))
    first = {}
    for p, span in enumerate(spans):
        for side, device in ((0, up), (1, down)):
            project(2, side * half, span, into(r1_send.at[side]))
            cols = slice(*span)
            first[side, p] = send(
                r1_send.at[side, :, cols],
                r1_recv.at[side, :, cols],
                r1_ssem.at[side, p],
                r1_rsem.at[side, p],
                device,
            )
    squares_sent = [share_squares(2, squares)]
    second = {}
    for side, k, device in ((0, 1, up), (1, ny - 1, down)):
        squares_sent.append(make_hidden(k))
        project(k, (1 - side) * half, (0, half), into(r2_send.at[side, 0]))
        second[side, 0] = send(
            r2_send.at[side, 0],
            r2_recv.at[side, 0],
            r2_ssem.at[side, 0],
            r2_rsem.at[side, 0],
            device,
        )
    make_hidden(0)
    for side in (0, 1):

        def store(cols, value, side=side):
            own_ref[:, side * half + cols.start : side * half + cols.stop] = value

        project(0, side * half, (0, half), store)
    for p, span in enumerate(last_spans):
        for side, k, device in ((0, 1, up), (1, ny - 1, down)):
            if p == 0:
                first[side, 0].wait_recv()
                first[side, 1].wait_recv()
            project(k, side * half, span, added(r2_send.at[side, 1], r1_recv.at[side]))
            cols = slice(*span)
            second[side, 1 + p] = send(
                r2_send.at[side, 1, :, cols],
                r2_recv.at[side, 1, :, cols],
                r2_ssem.at[side, 1 + p],
                r2_rsem.at[side, 1 + p],
                device,
            )
    for copy in squares_sent:
        copy.wait_recv()
    total_squares = ss_send[0]
    for k in range(ny - 1):
        total_squares = total_squares + ss_recv[k]
    scale = lax.rsqrt(as_column(total_squares[0:1, :], part) / DI + EPSILON)
    for side in (0, 1):
        second[side, 0].wait_recv()
        base = (1 - side) * half
        for c in range(0, half, 256):
            cols = slice(base + c, base + c + 256)
            own_ref[:, cols] = own_ref[:, cols] + r2_recv[side, 0, :, c : c + 256].astype(F32)
    leaving = []
    for p, span in enumerate(last_spans):
        for side in (0, 1):
            second[side, 1 + p].wait_recv()
            base = side * half
            for c in range(span[0], span[1], 256):
                cols = slice(base + c, base + c + 256)
                value = own_ref[:, cols] + r2_recv[side, 1, :, c : c + 256].astype(F32)
                out_v[:, cols] = (value * scale).astype(BF16)
            cols = slice(base + span[0], base + span[1])
            copy = pltpu.make_async_copy(
                out_v.at[:, cols], out_hbm.at[:, cols], out_sem.at[side, p]
            )
            copy.start()
            leaving.append(copy)
    for copy in sends + squares_sent + [*first.values(), *second.values()]:
        copy.wait_send()
    for copy in leaving:
        copy.wait()


def local(nx, nz, ny, stream, gate, inc, outc, step_raw, bias, rate, skip, gain, proj, starts):
    tokens, channels = stream.shape
    heads = step_raw.shape[0]
    state = inc.shape[1]
    width = proj.shape[1]
    half = width // 2
    sw = channels // 2
    sr = state // nz
    part = tokens // ny
    anyspace = pl.BlockSpec(memory_space=pl.ANY)
    dma = pltpu.SemaphoreType.DMA
    scratch = [
        pltpu.VMEM((1, heads), F32),
        pltpu.VMEM((1, heads), F32),
        pltpu.VMEM((1, heads), F32),
        pltpu.VMEM((channels,), F32),
        pltpu.VMEM((1, starts.shape[0]), jnp.int32),
        pltpu.VMEM((tokens, channels), BF16),
        pltpu.VMEM((tokens, channels), BF16),
        pltpu.VMEM((tokens, state), BF16),
        pltpu.VMEM((tokens, state), BF16),
        pltpu.VMEM((heads, tokens), F32),
        pltpu.VMEM((channels, width), BF16),
        pltpu.VMEM((LANE, tokens + LANE), F32),
        pltpu.VMEM((tokens + LANE, LANE), BF16),
        pltpu.VMEM((LANE, channels), BF16),
        pltpu.VMEM((tokens, channels), BF16),
        pltpu.VMEM((128, tokens), BF16),
        pltpu.VMEM((tokens, state), BF16),
        pltpu.VMEM((tokens, channels), F32),
        pltpu.VMEM((tokens, channels), F32),
        pltpu.VMEM((24, channels), F32),
        pltpu.VMEM((state, sw), F32),
        pltpu.VMEM((state + 8, sw), BF16),
        pltpu.VMEM((state + 8, sw), BF16),
        pltpu.VMEM((state, sw), F32),
        pltpu.VMEM((nz, sr, sw), BF16),
        pltpu.VMEM((nz, sr, sw), BF16),
        pltpu.VMEM((1, LANE), F32),
        pltpu.VMEM((nz, 1, LANE), F32),
        pltpu.VMEM((1, LANE), F32),
        pltpu.VMEM((nx, 1, LANE), F32),
        pltpu.VMEM((8, LANE), F32),
        pltpu.VMEM((8, sw), F32),
        pltpu.VMEM((1, sw), F32),
        pltpu.VMEM((nz, sr, sw), F32),
        pltpu.VMEM((8, sw), F32),
        pltpu.VMEM((sr, sw), BF16),
        pltpu.VMEM((nx, sr, sw), BF16),
        pltpu.VMEM((nz, sr, sw), BF16),
        pltpu.VMEM((nz, sr, sw), BF16),
        pltpu.VMEM((nz, sr, sw), BF16),
        pltpu.VMEM((nz, sr, sw), BF16),
        pltpu.VMEM((state, channels), BF16),
        pltpu.VMEM((tokens, channels), BF16),
        pltpu.VMEM((2, part, half), BF16),
        pltpu.VMEM((2, part, half), BF16),
        pltpu.VMEM((2, 2, part, half), BF16),
        pltpu.VMEM((2, 2, part, half), BF16),
        pltpu.VMEM((part, width), F32),
        pltpu.VMEM((part, width), BF16),
        pltpu.VMEM((ny, 8, part), F32),
        pltpu.VMEM((ny - 1, 8, part), F32),
        dma((5,)),
        dma((6,)),
        dma((2,)),
        dma((nz - 1,)),
        dma((nz - 1,)),
        dma((nx - 1,)),
        dma((nx - 1,)),
        dma((nz - 1,)),
        dma((nz - 1,)),
        dma((nx - 1,)),
        dma((nx - 1,)),
        dma((nz - 1,)),
        dma((nz - 1,)),
        dma((nz,)),
        dma((nz,)),
        dma((2, 2)),
        dma((2, 2)),
        dma((2, 3)),
        dma((2, 3)),
        dma((ny - 1,)),
        dma((ny - 1,)),
        dma((2, 2)),
    ]
    return pl.pallas_call(
        functools.partial(kernel, nx, nz, ny),
        out_shape=jax.ShapeDtypeStruct((part, width), BF16),
        in_specs=[anyspace] * 11,
        out_specs=anyspace,
        scratch_shapes=scratch,
        compiler_params=pltpu.CompilerParams(
            collective_id=0, has_side_effects=True, vmem_limit_bytes=56 * 1024 * 1024
        ),
        name="ssd_layer",
    )(
        stream,
        gate,
        inc,
        outc,
        step_raw,
        bias[None],
        rate[None],
        skip[None],
        gain,
        proj,
        starts[None],
    )


def solution(mesh):
    chips = mesh.shape["seq"] // 2
    nz = min(ALONG_Z, chips)
    in_specs = (
        P("seq", "head"),
        P("seq", "head"),
        P("seq", None),
        P("seq", None),
        P("head", "seq"),
        P("head"),
        P("head"),
        P("head"),
        P("head"),
        P("head", None),
        P(),
    )
    return jax.shard_map(
        functools.partial(local, chips // nz, nz, mesh.shape["head"]),
        mesh=mesh,
        in_specs=in_specs,
        out_specs=P(("seq", "head"), None),
        check_vma=False,
    )
```

```python
import functools

import jax
import jax.numpy as jnp
from jax import lax
from jax.experimental import pallas as pl
from jax.experimental.pallas import tpu as pltpu
from jax.sharding import PartitionSpec as P

DI = 5120
EPSILON = 1e-05
ALONG_Z = 8
LANE = 128
F32 = jnp.float32
BF16 = jnp.bfloat16
MESH = pl.DeviceIdType.MESH


def dot(a, b):
    return jnp.dot(a, b, preferred_element_type=F32)


def dot_nt(a, b):
    return lax.dot_general(a, b, (((1,), (1,)), ((), ())), preferred_element_type=F32)


def rounded(v):
    return v.astype(BF16).astype(F32)


def eye_mask(n):
    return lax.broadcasted_iota(jnp.int32, (n, n), 0) == lax.broadcasted_iota(jnp.int32, (n, n), 1)


def as_column(row, n):
    return jnp.sum(jnp.where(eye_mask(n), row, 0.0), axis=1, keepdims=True)


def as_row(column, n):
    return jnp.sum(jnp.where(eye_mask(n), column, 0.0), axis=0, keepdims=True)


def link_tile(row, rows):
    high = rounded(row)
    middle = rounded(row - high)
    low = row - high - middle
    at = lax.broadcasted_iota(jnp.int32, (rows, LANE), 0)
    return jnp.where(
        at == 0, high, jnp.where(at == 1, middle, jnp.where(at == 2, low, 0.0))
    ).astype(BF16)


def kernel(
    nx,
    nz,
    ny,
    x_hbm,
    g_hbm,
    b_hbm,
    c_hbm,
    st_hbm,
    bias_hbm,
    rate_hbm,
    skip_hbm,
    gain_hbm,
    w_hbm,
    doc_hbm,
    out_ref,
    bias_ref,
    rate_ref,
    skip_ref,
    gain_ref,
    doc_ref,
    x_v,
    g_v,
    b_v,
    c_v,
    st_v,
    w_v,
    m_ref,
    mt_ref,
    e_ref,
    v_ref,
    sc_ref,
    cj_ref,
    a1_ref,
    a2_ref,
    row_ref,
    own_s,
    pair_send,
    pair_recv,
    first_s,
    asend,
    arecv,
    zlog_send,
    zlog_recv,
    xlog_send,
    xlog_recv,
    ll_ref,
    lx_ref,
    l0_ref,
    pre_ref,
    pl_ref,
    xsend,
    xrecv,
    bsend,
    brecv,
    fsend,
    frecv,
    sp_ref,
    hid_ref,
    r1_send,
    r1_recv,
    r2_send,
    r2_recv,
    own_ref,
    ss_send,
    ss_recv,
    small_sem,
    copy_sem,
    p_sem,
    la_ssem,
    la_rsem,
    lx_ssem,
    lx_rsem,
    a_ssem,
    a_rsem,
    x_ssem,
    x_rsem,
    b_ssem,
    b_rsem,
    f_ssem,
    f_rsem,
    r1_ssem,
    r1_rsem,
    r2_ssem,
    r2_rsem,
    ss_ssem,
    ss_rsem,
):
    seq = lax.axis_index("seq")
    head = lax.axis_index("head")
    core = seq % 2
    z = (seq // 2) % nz
    xi = seq // (2 * nz)
    is_first = core == 0
    tokens, channels = x_v.shape
    heads = st_v.shape[0]
    state = b_v.shape[1]
    width = w_v.shape[1]
    half = width // 2
    side_width = channels // 2
    sr = state // nz
    part = tokens // ny
    offset = seq * tokens
    head_size = channels // heads

    barrier = pltpu.get_barrier_semaphore()
    partner = (seq + 1 - 2 * core, head)
    in_z = [((xi * nz + (z + k) % nz) * 2 + core, head) for k in range(nz)]
    in_x = [((((xi + k) % nx) * nz + z) * 2 + core, head) for k in range(nx)]
    in_y = [(seq, (head + k) % ny) for k in range(ny)]
    greeted = in_z[1:] + in_x[1:] + in_y[1:] + [partner]
    for device in greeted:
        pl.semaphore_signal(barrier, inc=1, device_id=device, device_id_type=MESH)

    small = [
        pltpu.make_async_copy(src, dst, small_sem.at[i])
        for i, (src, dst) in enumerate(
            (
                (doc_hbm, doc_ref),
                (bias_hbm, bias_ref),
                (rate_hbm, rate_ref),
                (skip_hbm, skip_ref),
                (gain_hbm, gain_ref),
            )
        )
    ]
    loads = [
        pltpu.make_async_copy(src, dst, copy_sem.at[i])
        for i, (src, dst) in enumerate(
            (
                (st_hbm, st_v),
                (b_hbm, b_v),
                (x_hbm, x_v),
                (c_hbm, c_v),
                (g_hbm, g_v),
                (w_hbm, w_v),
            )
        )
    ]
    for load in [loads[0], *small, *loads[1:3]]:
        load.start()

    def send(src, dst, ssem, rsem, device):
        copy = pltpu.make_async_remote_copy(
            src_ref=src,
            dst_ref=dst,
            send_sem=ssem,
            recv_sem=rsem,
            device_id=device,
            device_id_type=MESH,
        )
        copy.start()
        return copy

    def around(n):
        order = []
        for d in range(n // 2, 0, -1):
            order += [d] if 2 * d == n else [d, n - d]
        return order

    e_ref[...] = (
        (lax.broadcasted_iota(jnp.int32, (LANE, channels), 0) & 31)
        == lax.broadcasted_iota(jnp.int32, (LANE, channels), 1) // head_size
    ).astype(F32).astype(BF16)
    m_ref[...] = jnp.zeros_like(m_ref)
    ll_ref[...] = jnp.zeros_like(ll_ref)
    small[0].wait()
    starts = doc_ref[...]
    position = offset + lax.broadcasted_iota(jnp.int32, (tokens, 1), 0)
    doc_start = jnp.max(
        jnp.where(starts <= position, starts.astype(F32), -1.0), axis=1, keepdims=True
    )
    joined = doc_start < offset.astype(F32)
    last_start = doc_start[tokens - 1 :, :]

    for load in small[1:]:
        load.wait()
    bias = as_column(bias_ref[...], heads)
    rate = as_column(rate_ref[...], heads)
    skip = as_column(skip_ref[...], heads)
    loads[0].wait()
    step = st_v[...] + bias
    step = jnp.maximum(step, 0.0) + jnp.log1p(jnp.exp(-jnp.abs(step)))
    cum = -step * rate
    lane = lax.broadcasted_iota(jnp.int32, (heads, tokens), 1)
    shift = 1
    while shift < tokens:
        cum = cum + jnp.where(lane >= shift, pltpu.roll(cum, shift, 1), 0.0)
        shift *= 2
    mid = cum[:, tokens // 2 - 1 : tokens // 2]
    total = cum[:, tokens - 1 :]
    before_scale = jnp.exp(mid - cum) * step
    after_scale = jnp.exp(cum - mid)

    def put(first, columns, value):
        high = rounded(value)
        m_ref[first : first + heads, columns] = high
        m_ref[first + 32 : first + 32 + heads, columns] = value - high

    wide = (heads, LANE)
    put(0, slice(0, tokens), before_scale)
    put(64, slice(0, tokens), after_scale)
    put(0, slice(tokens, tokens + LANE), jnp.broadcast_to(jnp.exp(mid), wide))
    put(64, slice(tokens, tokens + LANE), jnp.broadcast_to(skip, wide))
    mt_ref[...] = m_ref[...].T.astype(BF16)
    gate_row = jnp.where(last_start < offset.astype(F32), total, -1e30)
    link_row = jnp.sum(
        jnp.where(
            lax.broadcasted_iota(jnp.int32, (heads, LANE), 0)
            == lax.broadcasted_iota(jnp.int32, (heads, LANE), 1),
            gate_row,
            0.0,
        ),
        axis=0,
        keepdims=True,
    )

    def expand(rows, upper):
        block = mt_ref[rows, :]
        at = lax.broadcasted_iota(jnp.int32, block.shape, 1)
        block = jnp.where((at >= 64) if upper else (at < 64), block.astype(F32), 0.0)
        return block.astype(BF16)

    row_ref[0:8, :] = dot(expand(slice(tokens - 8, tokens), True), e_ref[...])
    row_ref[8:16, :] = dot(expand(slice(tokens, tokens + 8), False), e_ref[...])
    row_ref[16:24, :] = dot(expand(slice(tokens, tokens + 8), True), e_ref[...])

    step_rows = 128
    columns = [slice(c, c + 256) for c in range(0, channels, 256)]
    cuts = [(c, min(256, side_width - c)) for c in range(0, side_width, 256)]
    mine = core * side_width
    others = (1 - core) * side_width

    def lanes(base, cut):
        return pl.ds(pl.multiple_of(base + cut[0], LANE), cut[1])

    loads[1].wait()
    kept = jnp.where(position.astype(F32) >= last_start, b_v[...].astype(F32), 0.0)
    kept = kept.T.astype(BF16)
    loads[2].wait()
    for load in loads[3:]:
        load.start()

    def summary(base, store):
        @pl.loop(0, tokens // step_rows)
        def _(i):
            rows = pl.ds(pl.multiple_of(i * step_rows, step_rows), step_rows)
            left = expand(rows, False)
            for cut in cuts:
                cols = lanes(base, cut)
                v_ref[rows, cols] = (
                    x_v[rows, cols].astype(F32) * dot(left, e_ref[:, cols])
                ).astype(BF16)

        for cut in cuts:
            cols = lanes(base, cut)
            store(
                slice(cut[0], cut[0] + cut[1]),
                dot(kept, v_ref[:, cols]) * row_ref[7:8, cols],
            )

    def to_partner(cols, value):
        pair_send[0:state, cols] = value.astype(BF16)

    def to_own(cols, value):
        own_s[:, cols] = value

    pair_send[state:, :] = jnp.zeros((8, side_width), BF16)
    pair_send[state:, 0:LANE] = link_tile(link_row, 8)
    summary(others, to_partner)
    pl.semaphore_wait(barrier, len(greeted))
    pair = send(pair_send, pair_recv, p_sem.at[0], p_sem.at[1], partner)
    summary(mine, to_own)

    def link_of(block):
        return jnp.sum(block.astype(F32), axis=0, keepdims=True)

    def spread(logs):
        at = lax.broadcasted_iota(jnp.int32, logs.shape, 1)
        value = jnp.where(at < heads, jnp.exp(logs), 0.0)
        high = value.astype(BF16)
        rest = value - high.astype(F32)
        middle = rest.astype(BF16)
        low = (rest - middle.astype(F32)).astype(BF16)
        hot = e_ref[:, pl.ds(pl.multiple_of(mine, LANE), side_width)]
        return dot(high, hot) + dot(middle, hot) + dot(low, hot)

    pair.wait_recv()
    partner_row = link_of(pair_recv[state:, 0:LANE])
    ll_ref[0:1, :] = jnp.where(is_first, link_row, partner_row)
    ll_ref[1:2, :] = jnp.where(is_first, partner_row, link_row)
    chip_log = link_row + partner_row
    pair_links = spread(ll_ref[0:8, :])
    l0_ref[...] = pair_links[0:1, :]
    zlog_send[...] = chip_log
    zlog_copies = {}
    for k in around(nz):
        zlog_copies[k] = send(
            zlog_send, zlog_recv.at[z], la_ssem.at[k - 1], la_rsem.at[k - 1], in_z[k]
        )
    zlog_recv[z] = chip_log
    row_copies = {}
    for k in [*around(nz), 0]:
        slot = (z + k) % nz
        rows = pl.ds(pl.multiple_of(slot * sr, sr), sr)
        own = own_s[rows, :]
        came = pair_recv[rows, :].astype(F32)
        earlier_core = jnp.where(is_first, own, came)
        first_s[rows, :] = earlier_core
        merged = pair_links[1:2, :] * earlier_core + jnp.where(is_first, came, own)
        if k:
            asend[slot] = merged.astype(BF16)
            row_copies[k] = send(
                asend.at[slot], arecv.at[z], a_ssem.at[k - 1], a_rsem.at[k - 1], in_z[k]
            )
        else:
            arecv[z] = merged.astype(BF16)

    loads[3].wait()
    cj_ref[...] = jnp.where(joined, c_v[...].astype(F32), 0.0).astype(BF16)
    loads[4].wait()

    def alone(first):
        rows = pl.ds(first, step_rows)
        scores = dot_nt(c_v[rows, :], b_v[...])
        at = offset + first + lax.broadcasted_iota(jnp.int32, (step_rows, 1), 0)
        source = offset + lax.broadcasted_iota(jnp.int32, (step_rows, tokens), 1)
        begun = jnp.max(
            jnp.where(starts <= at, starts.astype(F32), -1.0), axis=1, keepdims=True
        )
        live = (source <= at) & (source.astype(F32) >= begun)
        sc_ref[...] = jnp.where(live, scores, 0.0).astype(BF16)
        left = expand(rows, True)
        for cols in columns:
            scale = dot(left, e_ref[:, cols])
            gate = g_v[rows, cols].astype(F32)
            gate = gate / (1.0 + jnp.exp(-gate))
            inside = dot(sc_ref[...], v_ref[:, cols])
            skipped = row_ref[16:17, cols] * x_v[rows, cols].astype(F32)
            a1_ref[rows, cols] = scale * gate
            a2_ref[rows, cols] = (scale * inside + skipped) * gate

    @pl.loop(0, tokens // step_rows)
    def _(i):
        alone(pl.multiple_of(i * step_rows, step_rows))

    for k in around(nz):
        zlog_copies[k].wait_recv()
    for j in range(nz):
        ll_ref[j : j + 1, :] = zlog_recv[j]
    row_log = jnp.sum(ll_ref[0:nz, :], axis=0, keepdims=True)
    xlog_send[...] = row_log
    xlog_copies = {}
    for k in around(nx):
        xlog_copies[k] = send(
            xlog_send, xlog_recv.at[xi], lx_ssem.at[k - 1], lx_rsem.at[k - 1], in_x[k]
        )
    xlog_recv[xi] = row_log
    lx_ref[0:nz, :] = spread(ll_ref[0:nz, :])
    for k in around(nz):
        row_copies[k].wait_recv()
    prefix = jnp.zeros((sr, side_width), F32)
    product = jnp.ones((1, side_width), F32)
    for j in range(nz):
        pre_ref[j] = prefix
        pl_ref[j : j + 1, :] = product
        link = lx_ref[j : j + 1, :]
        prefix = link * prefix + arecv[j].astype(F32)
        product = product * link
    xsend[...] = prefix.astype(BF16)
    x_copies = {}
    for k in around(nx):
        x_copies[k] = send(
            xsend, xrecv.at[xi], x_ssem.at[k - 1], x_rsem.at[k - 1], in_x[k]
        )
    xrecv[xi] = xsend[...]
    for k in around(nx):
        xlog_copies[k].wait_recv()
    for j in range(nx):
        ll_ref[j : j + 1, :] = xlog_recv[j]
    lx_ref[0:nx, :] = spread(ll_ref[0:nx, :])
    for k in around(nx):
        x_copies[k].wait_recv()
    earlier = jnp.zeros((sr, side_width), F32)
    for j in range(nx - 1):
        after = lx_ref[j : j + 1, :] * earlier + xrecv[j].astype(F32)
        earlier = jnp.where(j < xi, after, earlier)
    back_copies = {}
    for k in [*around(nz), 0]:
        slot = (z + k) % nz
        value = (pre_ref[slot] + pl_ref[pl.ds(slot, 1), :] * earlier).astype(BF16)
        if k:
            bsend[slot] = value
            back_copies[k] = send(
                bsend.at[slot], brecv.at[z], b_ssem.at[k - 1], b_rsem.at[k - 1], in_z[k]
            )
        else:
            brecv[z] = value

    own_lanes = pl.ds(pl.multiple_of(mine, LANE), side_width)
    other_lanes = pl.ds(pl.multiple_of(others, LANE), side_width)
    final_copies = []
    for k in [0] + around(nz)[::-1]:
        if k:
            back_copies[k].wait_recv()
        slot = (z + nz - k) % nz
        rows = pl.ds(pl.multiple_of(slot * sr, sr), sr)
        to_first = brecv[slot].astype(F32)
        to_second = l0_ref[...] * to_first + first_s[rows, :]
        fsend[slot] = jnp.where(is_first, to_second, to_first).astype(BF16)
        final_copies.append(
            send(fsend.at[slot], frecv.at[slot], f_ssem.at[k], f_rsem.at[k], partner)
        )
        sp_ref[rows, own_lanes] = (
            row_ref[8:9, own_lanes] * jnp.where(is_first, to_first, to_second)
        ).astype(BF16)

    sends = [pair]
    for copies in (zlog_copies, row_copies, xlog_copies, x_copies, back_copies):
        sends += copies.values()
    sends += final_copies

    def chunk_rows(k):
        return pl.ds(pl.multiple_of(((head + k) % ny) * part, part), part)

    def hidden_columns(rows, cols):
        gated = a2_ref[rows, cols] + a1_ref[rows, cols] * dot(cj_ref[rows, :], sp_ref[:, cols])
        hid_ref[rows, cols] = (gated * gain_ref[cols].reshape(1, cols.size)).astype(BF16)
        return jnp.sum(gated * gated, axis=1, keepdims=True)

    def share_squares(k, squares):
        ss_send[k] = jnp.broadcast_to(as_row(squares, part), (8, part))
        if k:
            return send(
                ss_send.at[k],
                ss_recv.at[k - 1],
                ss_ssem.at[k - 1],
                ss_rsem.at[k - 1],
                in_y[k],
            )

    def make_hidden(k):
        rows = chunk_rows(k)
        squares = jnp.zeros((part, 1), F32)
        for cols in columns:
            squares = squares + hidden_columns(rows, pl.ds(cols.start, 256))
        return share_squares(k, squares)

    def project(k, base, span, store):
        rows = chunk_rows(k)
        for c in range(span[0], span[1], 256):
            store(
                slice(c, c + 256),
                dot(hid_ref[rows, :], w_v[:, base + c : base + c + 256]),
            )

    def into(ref):
        def store(cols, value):
            ref[:, cols] = value.astype(BF16)

        return store

    def added(ref, extra):
        def store(cols, value):
            ref[:, cols] = (value + extra[:, cols].astype(F32)).astype(BF16)

        return store

    far = chunk_rows(2)
    squares = jnp.zeros((part, 1), F32)
    for cut in cuts:
        squares = squares + hidden_columns(far, lanes(mine, cut))
    for copy in final_copies:
        copy.wait_recv()
    for j in range(nz):
        rows = slice(j * sr, (j + 1) * sr)
        sp_ref[rows, other_lanes] = (row_ref[8:9, other_lanes] * frecv[j].astype(F32)).astype(
            BF16
        )
    for cut in cuts:
        squares = squares + hidden_columns(far, lanes(others, cut))
    loads[5].wait()
    up, down = in_y[1], in_y[ny - 1]
    spans = ((0, 256), (256, half))
    last_spans = ((0, half - 256), (half - 256, half))
    first = {}
    for p, span in enumerate(spans):
        for side, device in ((0, up), (1, down)):
            project(2, side * half, span, into(r1_send.at[side]))
            cols = slice(*span)
            first[side, p] = send(
                r1_send.at[side, :, cols],
                r1_recv.at[side, :, cols],
                r1_ssem.at[side, p],
                r1_rsem.at[side, p],
                device,
            )
    squares_sent = [share_squares(2, squares)]
    second = {}
    for side, k, device in ((0, 1, up), (1, ny - 1, down)):
        squares_sent.append(make_hidden(k))
        project(k, (1 - side) * half, (0, half), into(r2_send.at[side, 0]))
        second[side, 0] = send(
            r2_send.at[side, 0],
            r2_recv.at[side, 0],
            r2_ssem.at[side, 0],
            r2_rsem.at[side, 0],
            device,
        )
    make_hidden(0)
    for side in (0, 1):

        def store(cols, value, side=side):
            own_ref[:, side * half + cols.start : side * half + cols.stop] = value

        project(0, side * half, (0, half), store)
    for p, span in enumerate(last_spans):
        for side, k, device in ((0, 1, up), (1, ny - 1, down)):
            if p == 0:
                first[side, 0].wait_recv()
                first[side, 1].wait_recv()
            project(k, side * half, span, added(r2_send.at[side, 1], r1_recv.at[side]))
            cols = slice(*span)
            second[side, 1 + p] = send(
                r2_send.at[side, 1, :, cols],
                r2_recv.at[side, 1, :, cols],
                r2_ssem.at[side, 1 + p],
                r2_rsem.at[side, 1 + p],
                device,
            )
    for copy in squares_sent:
        copy.wait_recv()
    total_squares = ss_send[0]
    for k in range(ny - 1):
        total_squares = total_squares + ss_recv[k]
    scale = lax.rsqrt(as_column(total_squares[0:1, :], part) / DI + EPSILON)
    for side in (0, 1):
        second[side, 0].wait_recv()
        base = (1 - side) * half
        for c in range(0, half, 256):
            cols = slice(base + c, base + c + 256)
            own_ref[:, cols] = own_ref[:, cols] + r2_recv[side, 0, :, c : c + 256].astype(F32)
    for p, span in enumerate(last_spans):
        for side in (0, 1):
            second[side, 1 + p].wait_recv()
            base = side * half
            for c in range(span[0], span[1], 256):
                cols = slice(base + c, base + c + 256)
                value = own_ref[:, cols] + r2_recv[side, 1, :, c : c + 256].astype(F32)
                out_ref[:, cols] = (value * scale).astype(BF16)
    for copy in sends + squares_sent + [*first.values(), *second.values()]:
        copy.wait_send()


def local(nx, nz, ny, stream, gate, inc, outc, step_raw, bias, rate, skip, gain, proj, starts):
    tokens, channels = stream.shape
    heads = step_raw.shape[0]
    state = inc.shape[1]
    width = proj.shape[1]
    half = width // 2
    sw = channels // 2
    sr = state // nz
    part = tokens // ny
    anyspace = pl.BlockSpec(memory_space=pl.ANY)
    dma = pltpu.SemaphoreType.DMA
    scratch = [
        pltpu.VMEM((1, heads), F32),
        pltpu.VMEM((1, heads), F32),
        pltpu.VMEM((1, heads), F32),
        pltpu.VMEM((channels,), F32),
        pltpu.VMEM((1, starts.shape[0]), jnp.int32),
        pltpu.VMEM((tokens, channels), BF16),
        pltpu.VMEM((tokens, channels), BF16),
        pltpu.VMEM((tokens, state), BF16),
        pltpu.VMEM((tokens, state), BF16),
        pltpu.VMEM((heads, tokens), F32),
        pltpu.VMEM((channels, width), BF16),
        pltpu.VMEM((LANE, tokens + LANE), F32),
        pltpu.VMEM((tokens + LANE, LANE), BF16),
        pltpu.VMEM((LANE, channels), BF16),
        pltpu.VMEM((tokens, channels), BF16),
        pltpu.VMEM((128, tokens), BF16),
        pltpu.VMEM((tokens, state), BF16),
        pltpu.VMEM((tokens, channels), F32),
        pltpu.VMEM((tokens, channels), F32),
        pltpu.VMEM((24, channels), F32),
        pltpu.VMEM((state, sw), F32),
        pltpu.VMEM((state + 8, sw), BF16),
        pltpu.VMEM((state + 8, sw), BF16),
        pltpu.VMEM((state, sw), F32),
        pltpu.VMEM((nz, sr, sw), BF16),
        pltpu.VMEM((nz, sr, sw), BF16),
        pltpu.VMEM((1, LANE), F32),
        pltpu.VMEM((nz, 1, LANE), F32),
        pltpu.VMEM((1, LANE), F32),
        pltpu.VMEM((nx, 1, LANE), F32),
        pltpu.VMEM((8, LANE), F32),
        pltpu.VMEM((8, sw), F32),
        pltpu.VMEM((1, sw), F32),
        pltpu.VMEM((nz, sr, sw), F32),
        pltpu.VMEM((8, sw), F32),
        pltpu.VMEM((sr, sw), BF16),
        pltpu.VMEM((nx, sr, sw), BF16),
        pltpu.VMEM((nz, sr, sw), BF16),
        pltpu.VMEM((nz, sr, sw), BF16),
        pltpu.VMEM((nz, sr, sw), BF16),
        pltpu.VMEM((nz, sr, sw), BF16),
        pltpu.VMEM((state, channels), BF16),
        pltpu.VMEM((tokens, channels), BF16),
        pltpu.VMEM((2, part, half), BF16),
        pltpu.VMEM((2, part, half), BF16),
        pltpu.VMEM((2, 2, part, half), BF16),
        pltpu.VMEM((2, 2, part, half), BF16),
        pltpu.VMEM((part, width), F32),
        pltpu.VMEM((ny, 8, part), F32),
        pltpu.VMEM((ny - 1, 8, part), F32),
        dma((5,)),
        dma((6,)),
        dma((2,)),
        dma((nz - 1,)),
        dma((nz - 1,)),
        dma((nx - 1,)),
        dma((nx - 1,)),
        dma((nz - 1,)),
        dma((nz - 1,)),
        dma((nx - 1,)),
        dma((nx - 1,)),
        dma((nz - 1,)),
        dma((nz - 1,)),
        dma((nz,)),
        dma((nz,)),
        dma((2, 2)),
        dma((2, 2)),
        dma((2, 3)),
        dma((2, 3)),
        dma((ny - 1,)),
        dma((ny - 1,)),
    ]
    return pl.pallas_call(
        functools.partial(kernel, nx, nz, ny),
        out_shape=pltpu.VMEM((part, width), BF16),
        in_specs=[anyspace] * 11,
        out_specs=pl.BlockSpec(memory_space=pltpu.VMEM),
        scratch_shapes=scratch,
        compiler_params=pltpu.CompilerParams(
            collective_id=0, has_side_effects=True, vmem_limit_bytes=56 * 1024 * 1024
        ),
        name="ssd_layer",
    )(
        stream,
        gate,
        inc,
        outc,
        step_raw,
        bias[None],
        rate[None],
        skip[None],
        gain,
        proj,
        starts[None],
    )


def solution(mesh):
    chips = mesh.shape["seq"] // 2
    nz = min(ALONG_Z, chips)
    in_specs = (
        P("seq", "head"),
        P("seq", "head"),
        P("seq", None),
        P("seq", None),
        P("head", "seq"),
        P("head"),
        P("head"),
        P("head"),
        P("head"),
        P("head", None),
        P(),
    )
    return jax.shard_map(
        functools.partial(local, chips // nz, nz, mesh.shape["head"]),
        mesh=mesh,
        in_specs=in_specs,
        out_specs=P(("seq", "head"), None),
        check_vma=False,
    )
```

```python
import functools

import jax
import jax.numpy as jnp
from jax import lax
from jax.experimental import pallas as pl
from jax.experimental.pallas import tpu as pltpu
from jax.sharding import PartitionSpec as P

DI = 5120
EPSILON = 1e-05
ALONG_Z = 8
LANE = 128
F32 = jnp.float32
BF16 = jnp.bfloat16
MESH = pl.DeviceIdType.MESH


def dot(a, b):
    return jnp.dot(a, b, preferred_element_type=F32)


def dot_nt(a, b):
    return lax.dot_general(a, b, (((1,), (1,)), ((), ())), preferred_element_type=F32)


def rounded(v):
    return v.astype(BF16).astype(F32)


def eye_mask(n):
    return lax.broadcasted_iota(jnp.int32, (n, n), 0) == lax.broadcasted_iota(jnp.int32, (n, n), 1)


def as_column(row, n):
    return jnp.sum(jnp.where(eye_mask(n), row, 0.0), axis=1, keepdims=True)


def as_row(column, n):
    return jnp.sum(jnp.where(eye_mask(n), column, 0.0), axis=0, keepdims=True)


def link_tile(row, rows):
    high = rounded(row)
    middle = rounded(row - high)
    low = row - high - middle
    at = lax.broadcasted_iota(jnp.int32, (rows, LANE), 0)
    return jnp.where(
        at == 0, high, jnp.where(at == 1, middle, jnp.where(at == 2, low, 0.0))
    ).astype(BF16)


def kernel(
    nx,
    nz,
    ny,
    x_hbm,
    g_hbm,
    b_hbm,
    c_hbm,
    st_hbm,
    bias_hbm,
    rate_hbm,
    skip_hbm,
    gain_hbm,
    w_hbm,
    doc_hbm,
    out_ref,
    bias_ref,
    rate_ref,
    skip_ref,
    gain_ref,
    doc_ref,
    x_v,
    g_v,
    b_v,
    c_v,
    st_v,
    w_v,
    m_ref,
    mt_ref,
    e_ref,
    v_ref,
    sc_ref,
    cj_ref,
    a1_ref,
    a2_ref,
    row_ref,
    own_s,
    pair_send,
    pair_recv,
    first_s,
    asend,
    arecv,
    zlog_send,
    zlog_recv,
    xlog_send,
    xlog_recv,
    ll_ref,
    lx_ref,
    l0_ref,
    pre_ref,
    pl_ref,
    xsend,
    xrecv,
    bsend,
    brecv,
    fsend,
    frecv,
    sp_ref,
    hid_ref,
    r1_send,
    r1_recv,
    r2_send,
    r2_recv,
    own_ref,
    ss_send,
    ss_recv,
    small_sem,
    copy_sem,
    p_sem,
    la_ssem,
    la_rsem,
    lx_ssem,
    lx_rsem,
    a_ssem,
    a_rsem,
    x_ssem,
    x_rsem,
    b_ssem,
    b_rsem,
    f_ssem,
    f_rsem,
    r1_ssem,
    r1_rsem,
    r2_ssem,
    r2_rsem,
    ss_ssem,
    ss_rsem,
):
    seq = lax.axis_index("seq")
    head = lax.axis_index("head")
    core = seq % 2
    z = (seq // 2) % nz
    xi = seq // (2 * nz)
    is_first = core == 0
    tokens, channels = x_v.shape
    heads = st_v.shape[0]
    state = b_v.shape[1]
    width = w_v.shape[1]
    half = width // 2
    side_width = channels // 2
    sr = state // nz
    part = tokens // ny
    offset = seq * tokens
    head_size = channels // heads

    barrier = pltpu.get_barrier_semaphore()
    partner = (seq + 1 - 2 * core, head)
    in_z = [((xi * nz + (z + k) % nz) * 2 + core, head) for k in range(nz)]
    in_x = [((((xi + k) % nx) * nz + z) * 2 + core, head) for k in range(nx)]
    in_y = [(seq, (head + k) % ny) for k in range(ny)]
    greeted = in_z[1:] + in_x[1:] + in_y[1:] + [partner]
    for device in greeted:
        pl.semaphore_signal(barrier, inc=1, device_id=device, device_id_type=MESH)

    small = [
        pltpu.make_async_copy(src, dst, small_sem.at[i])
        for i, (src, dst) in enumerate(
            (
                (doc_hbm, doc_ref),
                (bias_hbm, bias_ref),
                (rate_hbm, rate_ref),
                (skip_hbm, skip_ref),
                (gain_hbm, gain_ref),
            )
        )
    ]
    loads = [
        pltpu.make_async_copy(src, dst, copy_sem.at[i])
        for i, (src, dst) in enumerate(
            (
                (st_hbm, st_v),
                (b_hbm, b_v),
                (x_hbm, x_v),
                (c_hbm, c_v),
                (g_hbm, g_v),
                (w_hbm, w_v),
            )
        )
    ]
    for load in [loads[0], *small, *loads[1:3]]:
        load.start()

    def send(src, dst, ssem, rsem, device):
        copy = pltpu.make_async_remote_copy(
            src_ref=src,
            dst_ref=dst,
            send_sem=ssem,
            recv_sem=rsem,
            device_id=device,
            device_id_type=MESH,
        )
        copy.start()
        return copy

    def around(n):
        order = []
        for d in range(n // 2, 0, -1):
            order += [d] if 2 * d == n else [d, n - d]
        return order

    e_ref[...] = (
        (lax.broadcasted_iota(jnp.int32, (LANE, channels), 0) & 31)
        == lax.broadcasted_iota(jnp.int32, (LANE, channels), 1) // head_size
    ).astype(F32).astype(BF16)
    m_ref[...] = jnp.zeros_like(m_ref)
    ll_ref[...] = jnp.zeros_like(ll_ref)
    small[0].wait()
    starts = doc_ref[...]
    position = offset + lax.broadcasted_iota(jnp.int32, (tokens, 1), 0)
    doc_start = jnp.max(
        jnp.where(starts <= position, starts.astype(F32), -1.0), axis=1, keepdims=True
    )
    joined = doc_start < offset.astype(F32)
    last_start = doc_start[tokens - 1 :, :]

    for load in small[1:]:
        load.wait()
    bias = as_column(bias_ref[...], heads)
    rate = as_column(rate_ref[...], heads)
    skip = as_column(skip_ref[...], heads)
    loads[0].wait()
    step = st_v[...] + bias
    step = jnp.maximum(step, 0.0) + jnp.log1p(jnp.exp(-jnp.abs(step)))
    cum = -step * rate
    lane = lax.broadcasted_iota(jnp.int32, (heads, tokens), 1)
    shift = 1
    while shift < tokens:
        cum = cum + jnp.where(lane >= shift, pltpu.roll(cum, shift, 1), 0.0)
        shift *= 2
    mid = cum[:, tokens // 2 - 1 : tokens // 2]
    total = cum[:, tokens - 1 :]
    before_scale = jnp.exp(mid - cum) * step
    after_scale = jnp.exp(cum - mid)

    def put(first, columns, value):
        high = rounded(value)
        m_ref[first : first + heads, columns] = high
        m_ref[first + 32 : first + 32 + heads, columns] = value - high

    wide = (heads, LANE)
    put(0, slice(0, tokens), before_scale)
    put(64, slice(0, tokens), after_scale)
    put(0, slice(tokens, tokens + LANE), jnp.broadcast_to(jnp.exp(mid), wide))
    put(64, slice(tokens, tokens + LANE), jnp.broadcast_to(skip, wide))
    mt_ref[...] = m_ref[...].T.astype(BF16)
    gate_row = jnp.where(last_start < offset.astype(F32), total, -1e30)
    link_row = jnp.sum(
        jnp.where(
            lax.broadcasted_iota(jnp.int32, (heads, LANE), 0)
            == lax.broadcasted_iota(jnp.int32, (heads, LANE), 1),
            gate_row,
            0.0,
        ),
        axis=0,
        keepdims=True,
    )

    def expand(rows, upper):
        block = mt_ref[rows, :]
        at = lax.broadcasted_iota(jnp.int32, block.shape, 1)
        block = jnp.where((at >= 64) if upper else (at < 64), block.astype(F32), 0.0)
        return block.astype(BF16)

    row_ref[0:8, :] = dot(expand(slice(tokens - 8, tokens), True), e_ref[...])
    row_ref[8:16, :] = dot(expand(slice(tokens, tokens + 8), False), e_ref[...])
    row_ref[16:24, :] = dot(expand(slice(tokens, tokens + 8), True), e_ref[...])

    step_rows = 128
    columns = [slice(c, c + 256) for c in range(0, channels, 256)]
    cuts = [(c, min(256, side_width - c)) for c in range(0, side_width, 256)]
    mine = core * side_width
    others = (1 - core) * side_width

    def lanes(base, cut):
        return pl.ds(pl.multiple_of(base + cut[0], LANE), cut[1])

    loads[1].wait()
    kept = jnp.where(position.astype(F32) >= last_start, b_v[...].astype(F32), 0.0)
    kept = kept.T.astype(BF16)
    loads[2].wait()
    for load in loads[3:]:
        load.start()

    def summary(base, store):
        @pl.loop(0, tokens // step_rows)
        def _(i):
            rows = pl.ds(pl.multiple_of(i * step_rows, step_rows), step_rows)
            left = expand(rows, False)
            for cut in cuts:
                cols = lanes(base, cut)
                v_ref[rows, cols] = (
                    x_v[rows, cols].astype(F32) * dot(left, e_ref[:, cols])
                ).astype(BF16)

        for cut in cuts:
            cols = lanes(base, cut)
            store(
                slice(cut[0], cut[0] + cut[1]),
                dot(kept, v_ref[:, cols]) * row_ref[7:8, cols],
            )

    def to_partner(cols, value):
        pair_send[0:state, cols] = value.astype(BF16)

    def to_own(cols, value):
        own_s[:, cols] = value

    pair_send[state:, :] = jnp.zeros((8, side_width), BF16)
    pair_send[state:, 0:LANE] = link_tile(link_row, 8)
    summary(others, to_partner)
    pl.semaphore_wait(barrier, len(greeted))
    pair = send(pair_send, pair_recv, p_sem.at[0], p_sem.at[1], partner)
    summary(mine, to_own)

    def link_of(block):
        return jnp.sum(block.astype(F32), axis=0, keepdims=True)

    def spread(logs):
        at = lax.broadcasted_iota(jnp.int32, logs.shape, 1)
        value = jnp.where(at < heads, jnp.exp(logs), 0.0)
        high = value.astype(BF16)
        rest = value - high.astype(F32)
        middle = rest.astype(BF16)
        low = (rest - middle.astype(F32)).astype(BF16)
        hot = e_ref[:, pl.ds(pl.multiple_of(mine, LANE), side_width)]
        return dot(high, hot) + dot(middle, hot) + dot(low, hot)

    pair.wait_recv()
    partner_row = link_of(pair_recv[state:, 0:LANE])
    ll_ref[0:1, :] = jnp.where(is_first, link_row, partner_row)
    ll_ref[1:2, :] = jnp.where(is_first, partner_row, link_row)
    chip_log = link_row + partner_row
    pair_links = spread(ll_ref[0:8, :])
    l0_ref[...] = pair_links[0:1, :]
    zlog_send[...] = chip_log
    zlog_copies = {}
    for k in around(nz):
        zlog_copies[k] = send(
            zlog_send, zlog_recv.at[z], la_ssem.at[k - 1], la_rsem.at[k - 1], in_z[k]
        )
    zlog_recv[z] = chip_log
    row_copies = {}
    cut_at = (side_width * 3 // 5) // LANE * LANE
    groups = (slice(0, cut_at), slice(cut_at, side_width))

    def send_out(g, k, slot):
        row_copies[g, k] = send(
            asend.at[slot, :, groups[g]],
            arecv.at[z, :, groups[g]],
            a_ssem.at[g, k - 1],
            a_rsem.at[g, k - 1],
            in_z[k],
        )

    for k in [*around(nz), 0]:
        slot = (z + k) % nz
        rows = pl.ds(pl.multiple_of(slot * sr, sr), sr)
        own = own_s[rows, :]
        came = pair_recv[rows, :].astype(F32)
        earlier_core = jnp.where(is_first, own, came)
        first_s[rows, :] = earlier_core
        merged = pair_links[1:2, :] * earlier_core + jnp.where(is_first, came, own)
        if k:
            asend[slot] = merged.astype(BF16)
            send_out(0, k, slot)
        else:
            arecv[z] = merged.astype(BF16)
    for k in around(nz):
        send_out(1, k, (z + k) % nz)

    loads[3].wait()
    cj_ref[...] = jnp.where(joined, c_v[...].astype(F32), 0.0).astype(BF16)
    loads[4].wait()

    def alone(first):
        rows = pl.ds(first, step_rows)
        scores = dot_nt(c_v[rows, :], b_v[...])
        at = offset + first + lax.broadcasted_iota(jnp.int32, (step_rows, 1), 0)
        source = offset + lax.broadcasted_iota(jnp.int32, (step_rows, tokens), 1)
        begun = jnp.max(
            jnp.where(starts <= at, starts.astype(F32), -1.0), axis=1, keepdims=True
        )
        live = (source <= at) & (source.astype(F32) >= begun)
        sc_ref[...] = jnp.where(live, scores, 0.0).astype(BF16)
        left = expand(rows, True)
        for cols in columns:
            scale = dot(left, e_ref[:, cols])
            gate = g_v[rows, cols].astype(F32)
            gate = gate / (1.0 + jnp.exp(-gate))
            inside = dot(sc_ref[...], v_ref[:, cols])
            skipped = row_ref[16:17, cols] * x_v[rows, cols].astype(F32)
            a1_ref[rows, cols] = scale * gate
            a2_ref[rows, cols] = (scale * inside + skipped) * gate

    @pl.loop(0, tokens // step_rows)
    def _(i):
        alone(pl.multiple_of(i * step_rows, step_rows))

    for k in around(nz):
        zlog_copies[k].wait_recv()
    for j in range(nz):
        ll_ref[j : j + 1, :] = zlog_recv[j]
    row_log = jnp.sum(ll_ref[0:nz, :], axis=0, keepdims=True)
    xlog_send[...] = row_log
    xlog_copies = {}
    for k in around(nx):
        xlog_copies[k] = send(
            xlog_send, xlog_recv.at[xi], lx_ssem.at[k - 1], lx_rsem.at[k - 1], in_x[k]
        )
    xlog_recv[xi] = row_log
    lx_ref[0:nz, :] = spread(ll_ref[0:nz, :])
    x_copies = {}
    for g, cols in enumerate(groups):
        for k in around(nz):
            row_copies[g, k].wait_recv()
        prefix = jnp.zeros((sr, cols.stop - cols.start), F32)
        product = jnp.ones((1, cols.stop - cols.start), F32)
        for j in range(nz):
            pre_ref[j, :, cols] = prefix
            pl_ref[j : j + 1, cols] = product
            link = lx_ref[j : j + 1, cols]
            prefix = link * prefix + arecv[j, :, cols].astype(F32)
            product = product * link
        xsend[:, cols] = prefix.astype(BF16)
        for k in around(nx):
            x_copies[g, k] = send(
                xsend.at[:, cols],
                xrecv.at[xi, :, cols],
                x_ssem.at[g, k - 1],
                x_rsem.at[g, k - 1],
                in_x[k],
            )
        xrecv[xi, :, cols] = xsend[:, cols]
    for k in around(nx):
        xlog_copies[k].wait_recv()
    for j in range(nx):
        ll_ref[j : j + 1, :] = xlog_recv[j]
    lx_ref[0:nx, :] = spread(ll_ref[0:nx, :])
    back_copies = {}
    for g, cols in enumerate(groups):
        for k in around(nx):
            x_copies[g, k].wait_recv()
        earlier = jnp.zeros((sr, cols.stop - cols.start), F32)
        for j in range(nx - 1):
            after = lx_ref[j : j + 1, cols] * earlier + xrecv[j, :, cols].astype(F32)
            earlier = jnp.where(j < xi, after, earlier)
        for k in [*around(nz), 0]:
            slot = (z + k) % nz
            value = (pre_ref[slot, :, cols] + pl_ref[pl.ds(slot, 1), cols] * earlier).astype(BF16)
            if k:
                bsend[slot, :, cols] = value
                back_copies[g, k] = send(
                    bsend.at[slot, :, cols],
                    brecv.at[z, :, cols],
                    b_ssem.at[g, k - 1],
                    b_rsem.at[g, k - 1],
                    in_z[k],
                )
            else:
                brecv[z, :, cols] = value

    other_lanes = pl.ds(pl.multiple_of(others, LANE), side_width)
    final_copies = []
    for g, cols in enumerate(groups):
        own_lanes = pl.ds(pl.multiple_of(mine + cols.start, LANE), cols.stop - cols.start)
        for k in [0] + around(nz)[::-1]:
            if k:
                back_copies[g, k].wait_recv()
            slot = (z + nz - k) % nz
            rows = pl.ds(pl.multiple_of(slot * sr, sr), sr)
            to_first = brecv[slot, :, cols].astype(F32)
            to_second = l0_ref[:, cols] * to_first + first_s[rows, cols]
            fsend[slot, :, cols] = jnp.where(is_first, to_second, to_first).astype(BF16)
            final_copies.append(
                send(
                    fsend.at[slot, :, cols],
                    frecv.at[slot, :, cols],
                    f_ssem.at[g, k],
                    f_rsem.at[g, k],
                    partner,
                )
            )
            sp_ref[rows, own_lanes] = (
                row_ref[8:9, own_lanes] * jnp.where(is_first, to_first, to_second)
            ).astype(BF16)

    sends = [pair]
    for copies in (zlog_copies, row_copies, xlog_copies, x_copies, back_copies):
        sends += copies.values()
    sends += final_copies

    def chunk_rows(k):
        return pl.ds(pl.multiple_of(((head + k) % ny) * part, part), part)

    def hidden_columns(rows, cols):
        gated = a2_ref[rows, cols] + a1_ref[rows, cols] * dot(cj_ref[rows, :], sp_ref[:, cols])
        hid_ref[rows, cols] = (gated * gain_ref[cols].reshape(1, cols.size)).astype(BF16)
        return jnp.sum(gated * gated, axis=1, keepdims=True)

    def share_squares(k, squares):
        ss_send[k] = jnp.broadcast_to(as_row(squares, part), (8, part))
        if k:
            return send(
                ss_send.at[k],
                ss_recv.at[k - 1],
                ss_ssem.at[k - 1],
                ss_rsem.at[k - 1],
                in_y[k],
            )

    def make_hidden(k):
        rows = chunk_rows(k)
        squares = jnp.zeros((part, 1), F32)
        for cols in columns:
            squares = squares + hidden_columns(rows, pl.ds(cols.start, 256))
        return share_squares(k, squares)

    def project(k, base, span, store):
        rows = chunk_rows(k)
        for c in range(span[0], span[1], 256):
            store(
                slice(c, c + 256),
                dot(hid_ref[rows, :], w_v[:, base + c : base + c + 256]),
            )

    def into(ref):
        def store(cols, value):
            ref[:, cols] = value.astype(BF16)

        return store

    def added(ref, extra):
        def store(cols, value):
            ref[:, cols] = (value + extra[:, cols].astype(F32)).astype(BF16)

        return store

    far = chunk_rows(2)
    squares = jnp.zeros((part, 1), F32)
    for cut in cuts:
        squares = squares + hidden_columns(far, lanes(mine, cut))
    for copy in final_copies:
        copy.wait_recv()
    for j in range(nz):
        rows = slice(j * sr, (j + 1) * sr)
        sp_ref[rows, other_lanes] = (row_ref[8:9, other_lanes] * frecv[j].astype(F32)).astype(
            BF16
        )
    for cut in cuts:
        squares = squares + hidden_columns(far, lanes(others, cut))
    loads[5].wait()
    up, down = in_y[1], in_y[ny - 1]
    spans = ((0, 256), (256, half))
    last_spans = ((0, half - 256), (half - 256, half))
    first = {}
    for p, span in enumerate(spans):
        for side, device in ((0, up), (1, down)):
            project(2, side * half, span, into(r1_send.at[side]))
            cols = slice(*span)
            first[side, p] = send(
                r1_send.at[side, :, cols],
                r1_recv.at[side, :, cols],
                r1_ssem.at[side, p],
                r1_rsem.at[side, p],
                device,
            )
    squares_sent = [share_squares(2, squares)]
    second = {}
    for side, k, device in ((0, 1, up), (1, ny - 1, down)):
        squares_sent.append(make_hidden(k))
        project(k, (1 - side) * half, (0, half), into(r2_send.at[side, 0]))
        second[side, 0] = send(
            r2_send.at[side, 0],
            r2_recv.at[side, 0],
            r2_ssem.at[side, 0],
            r2_rsem.at[side, 0],
            device,
        )
    make_hidden(0)
    for side in (0, 1):

        def store(cols, value, side=side):
            own_ref[:, side * half + cols.start : side * half + cols.stop] = value

        project(0, side * half, (0, half), store)
    for p, span in enumerate(last_spans):
        for side, k, device in ((0, 1, up), (1, ny - 1, down)):
            if p == 0:
                first[side, 0].wait_recv()
                first[side, 1].wait_recv()
            project(k, side * half, span, added(r2_send.at[side, 1], r1_recv.at[side]))
            cols = slice(*span)
            second[side, 1 + p] = send(
                r2_send.at[side, 1, :, cols],
                r2_recv.at[side, 1, :, cols],
                r2_ssem.at[side, 1 + p],
                r2_rsem.at[side, 1 + p],
                device,
            )
    for copy in squares_sent:
        copy.wait_recv()
    total_squares = ss_send[0]
    for k in range(ny - 1):
        total_squares = total_squares + ss_recv[k]
    scale = lax.rsqrt(as_column(total_squares[0:1, :], part) / DI + EPSILON)
    for side in (0, 1):
        second[side, 0].wait_recv()
        base = (1 - side) * half
        for c in range(0, half, 256):
            cols = slice(base + c, base + c + 256)
            own_ref[:, cols] = own_ref[:, cols] + r2_recv[side, 0, :, c : c + 256].astype(F32)
    for p, span in enumerate(last_spans):
        for side in (0, 1):
            second[side, 1 + p].wait_recv()
            base = side * half
            for c in range(span[0], span[1], 256):
                cols = slice(base + c, base + c + 256)
                value = own_ref[:, cols] + r2_recv[side, 1, :, c : c + 256].astype(F32)
                out_ref[:, cols] = (value * scale).astype(BF16)
    for copy in sends + squares_sent + [*first.values(), *second.values()]:
        copy.wait_send()


def local(nx, nz, ny, stream, gate, inc, outc, step_raw, bias, rate, skip, gain, proj, starts):
    tokens, channels = stream.shape
    heads = step_raw.shape[0]
    state = inc.shape[1]
    width = proj.shape[1]
    half = width // 2
    sw = channels // 2
    sr = state // nz
    part = tokens // ny
    anyspace = pl.BlockSpec(memory_space=pl.ANY)
    dma = pltpu.SemaphoreType.DMA
    scratch = [
        pltpu.VMEM((1, heads), F32),
        pltpu.VMEM((1, heads), F32),
        pltpu.VMEM((1, heads), F32),
        pltpu.VMEM((channels,), F32),
        pltpu.VMEM((1, starts.shape[0]), jnp.int32),
        pltpu.VMEM((tokens, channels), BF16),
        pltpu.VMEM((tokens, channels), BF16),
        pltpu.VMEM((tokens, state), BF16),
        pltpu.VMEM((tokens, state), BF16),
        pltpu.VMEM((heads, tokens), F32),
        pltpu.VMEM((channels, width), BF16),
        pltpu.VMEM((LANE, tokens + LANE), F32),
        pltpu.VMEM((tokens + LANE, LANE), BF16),
        pltpu.VMEM((LANE, channels), BF16),
        pltpu.VMEM((tokens, channels), BF16),
        pltpu.VMEM((128, tokens), BF16),
        pltpu.VMEM((tokens, state), BF16),
        pltpu.VMEM((tokens, channels), F32),
        pltpu.VMEM((tokens, channels), F32),
        pltpu.VMEM((24, channels), F32),
        pltpu.VMEM((state, sw), F32),
        pltpu.VMEM((state + 8, sw), BF16),
        pltpu.VMEM((state + 8, sw), BF16),
        pltpu.VMEM((state, sw), F32),
        pltpu.VMEM((nz, sr, sw), BF16),
        pltpu.VMEM((nz, sr, sw), BF16),
        pltpu.VMEM((1, LANE), F32),
        pltpu.VMEM((nz, 1, LANE), F32),
        pltpu.VMEM((1, LANE), F32),
        pltpu.VMEM((nx, 1, LANE), F32),
        pltpu.VMEM((8, LANE), F32),
        pltpu.VMEM((8, sw), F32),
        pltpu.VMEM((1, sw), F32),
        pltpu.VMEM((nz, sr, sw), F32),
        pltpu.VMEM((8, sw), F32),
        pltpu.VMEM((sr, sw), BF16),
        pltpu.VMEM((nx, sr, sw), BF16),
        pltpu.VMEM((nz, sr, sw), BF16),
        pltpu.VMEM((nz, sr, sw), BF16),
        pltpu.VMEM((nz, sr, sw), BF16),
        pltpu.VMEM((nz, sr, sw), BF16),
        pltpu.VMEM((state, channels), BF16),
        pltpu.VMEM((tokens, channels), BF16),
        pltpu.VMEM((2, part, half), BF16),
        pltpu.VMEM((2, part, half), BF16),
        pltpu.VMEM((2, 2, part, half), BF16),
        pltpu.VMEM((2, 2, part, half), BF16),
        pltpu.VMEM((part, width), F32),
        pltpu.VMEM((ny, 8, part), F32),
        pltpu.VMEM((ny - 1, 8, part), F32),
        dma((5,)),
        dma((6,)),
        dma((2,)),
        dma((nz - 1,)),
        dma((nz - 1,)),
        dma((nx - 1,)),
        dma((nx - 1,)),
        dma((2, nz - 1)),
        dma((2, nz - 1)),
        dma((2, nx - 1)),
        dma((2, nx - 1)),
        dma((2, nz - 1)),
        dma((2, nz - 1)),
        dma((2, nz)),
        dma((2, nz)),
        dma((2, 2)),
        dma((2, 2)),
        dma((2, 3)),
        dma((2, 3)),
        dma((ny - 1,)),
        dma((ny - 1,)),
    ]
    return pl.pallas_call(
        functools.partial(kernel, nx, nz, ny),
        out_shape=pltpu.VMEM((part, width), BF16),
        in_specs=[anyspace] * 11,
        out_specs=pl.BlockSpec(memory_space=pltpu.VMEM),
        scratch_shapes=scratch,
        compiler_params=pltpu.CompilerParams(
            collective_id=0, has_side_effects=True, vmem_limit_bytes=56 * 1024 * 1024
        ),
        name="ssd_layer",
    )(
        stream,
        gate,
        inc,
        outc,
        step_raw,
        bias[None],
        rate[None],
        skip[None],
        gain,
        proj,
        starts[None],
    )


def solution(mesh):
    chips = mesh.shape["seq"] // 2
    nz = min(ALONG_Z, chips)
    in_specs = (
        P("seq", "head"),
        P("seq", "head"),
        P("seq", None),
        P("seq", None),
        P("head", "seq"),
        P("head"),
        P("head"),
        P("head"),
        P("head"),
        P("head", None),
        P(),
    )
    return jax.shard_map(
        functools.partial(local, chips // nz, nz, mesh.shape["head"]),
        mesh=mesh,
        in_specs=in_specs,
        out_specs=P(("seq", "head"), None),
        check_vma=False,
    )
```

```python
import functools

import jax
import jax.numpy as jnp
from jax import lax
from jax.experimental import pallas as pl
from jax.experimental.pallas import tpu as pltpu
from jax.sharding import PartitionSpec as P

DI = 5120
EPSILON = 1e-05
ALONG_Z = 8
LANE = 128
F32 = jnp.float32
BF16 = jnp.bfloat16
MESH = pl.DeviceIdType.MESH


def dot(a, b):
    return jnp.dot(a, b, preferred_element_type=F32)


def dot_nt(a, b):
    return lax.dot_general(a, b, (((1,), (1,)), ((), ())), preferred_element_type=F32)


def rounded(v):
    return v.astype(BF16).astype(F32)


def eye_mask(n):
    return lax.broadcasted_iota(jnp.int32, (n, n), 0) == lax.broadcasted_iota(jnp.int32, (n, n), 1)


def as_column(row, n):
    return jnp.sum(jnp.where(eye_mask(n), row, 0.0), axis=1, keepdims=True)


def as_row(column, n):
    return jnp.sum(jnp.where(eye_mask(n), column, 0.0), axis=0, keepdims=True)


def link_tile(row, rows):
    high = rounded(row)
    middle = rounded(row - high)
    low = row - high - middle
    at = lax.broadcasted_iota(jnp.int32, (rows, LANE), 0)
    return jnp.where(
        at == 0, high, jnp.where(at == 1, middle, jnp.where(at == 2, low, 0.0))
    ).astype(BF16)


def kernel(
    nx,
    nz,
    ny,
    x_hbm,
    g_hbm,
    b_hbm,
    c_hbm,
    st_hbm,
    bias_hbm,
    rate_hbm,
    skip_hbm,
    gain_hbm,
    w_hbm,
    doc_hbm,
    out_ref,
    bias_ref,
    rate_ref,
    skip_ref,
    gain_ref,
    doc_ref,
    x_v,
    g_v,
    b_v,
    c_v,
    st_v,
    w_v,
    m_ref,
    mt_ref,
    e_ref,
    v_ref,
    sc_ref,
    cj_ref,
    a1_ref,
    a2_ref,
    row_ref,
    own_s,
    pair_send,
    pair_recv,
    first_s,
    asend,
    arecv,
    zlog_send,
    zlog_recv,
    xlog_send,
    xlog_recv,
    ll_ref,
    lx_ref,
    l0_ref,
    pre_ref,
    pl_ref,
    xsend,
    xrecv,
    bsend,
    brecv,
    fsend,
    frecv,
    sp_ref,
    hid_ref,
    r1_send,
    r1_recv,
    r2_send,
    r2_recv,
    own_ref,
    ss_send,
    ss_recv,
    small_sem,
    copy_sem,
    p_sem,
    la_ssem,
    la_rsem,
    lx_ssem,
    lx_rsem,
    a_ssem,
    a_rsem,
    x_ssem,
    x_rsem,
    b_ssem,
    b_rsem,
    f_ssem,
    f_rsem,
    r1_ssem,
    r1_rsem,
    r2_ssem,
    r2_rsem,
    ss_ssem,
    ss_rsem,
):
    seq = lax.axis_index("seq")
    head = lax.axis_index("head")
    core = seq % 2
    z = (seq // 2) % nz
    xi = seq // (2 * nz)
    is_first = core == 0
    tokens, channels = x_v.shape
    heads = st_v.shape[0]
    state = b_v.shape[1]
    width = w_v.shape[1]
    half = width // 2
    side_width = channels // 2
    sr = state // nz
    part = tokens // ny
    offset = seq * tokens
    head_size = channels // heads

    barrier = pltpu.get_barrier_semaphore()
    partner = (seq + 1 - 2 * core, head)
    in_z = [((xi * nz + (z + k) % nz) * 2 + core, head) for k in range(nz)]
    in_x = [((((xi + k) % nx) * nz + z) * 2 + core, head) for k in range(nx)]
    in_y = [(seq, (head + k) % ny) for k in range(ny)]
    greeted = in_z[1:] + in_x[1:] + in_y[1:] + [partner]
    for device in greeted:
        pl.semaphore_signal(barrier, inc=1, device_id=device, device_id_type=MESH)

    small = [
        pltpu.make_async_copy(src, dst, small_sem.at[i])
        for i, (src, dst) in enumerate(
            (
                (doc_hbm, doc_ref),
                (bias_hbm, bias_ref),
                (rate_hbm, rate_ref),
                (skip_hbm, skip_ref),
                (gain_hbm, gain_ref),
            )
        )
    ]
    loads = [
        pltpu.make_async_copy(src, dst, copy_sem.at[i])
        for i, (src, dst) in enumerate(
            (
                (st_hbm, st_v),
                (b_hbm, b_v),
                (x_hbm, x_v),
                (c_hbm, c_v),
                (g_hbm, g_v),
                (w_hbm, w_v),
            )
        )
    ]
    for load in [loads[0], *small, *loads[1:3]]:
        load.start()

    def send(src, dst, ssem, rsem, device):
        copy = pltpu.make_async_remote_copy(
            src_ref=src,
            dst_ref=dst,
            send_sem=ssem,
            recv_sem=rsem,
            device_id=device,
            device_id_type=MESH,
        )
        copy.start()
        return copy

    def around(n):
        order = []
        for d in range(n // 2, 0, -1):
            order += [d] if 2 * d == n else [d, n - d]
        return order

    e_ref[...] = (
        (lax.broadcasted_iota(jnp.int32, (LANE, channels), 0) & 31)
        == lax.broadcasted_iota(jnp.int32, (LANE, channels), 1) // head_size
    ).astype(F32).astype(BF16)
    m_ref[...] = jnp.zeros_like(m_ref)
    ll_ref[...] = jnp.zeros_like(ll_ref)
    small[0].wait()
    starts = doc_ref[...]
    position = offset + lax.broadcasted_iota(jnp.int32, (tokens, 1), 0)
    doc_start = jnp.max(
        jnp.where(starts <= position, starts.astype(F32), -1.0), axis=1, keepdims=True
    )
    joined = doc_start < offset.astype(F32)
    last_start = doc_start[tokens - 1 :, :]

    for load in small[1:]:
        load.wait()
    bias = as_column(bias_ref[...], heads)
    rate = as_column(rate_ref[...], heads)
    skip = as_column(skip_ref[...], heads)
    loads[0].wait()
    step = st_v[...] + bias
    step = jnp.maximum(step, 0.0) + jnp.log1p(jnp.exp(-jnp.abs(step)))
    cum = -step * rate
    lane = lax.broadcasted_iota(jnp.int32, (heads, tokens), 1)
    shift = 1
    while shift < tokens:
        cum = cum + jnp.where(lane >= shift, pltpu.roll(cum, shift, 1), 0.0)
        shift *= 2
    mid = cum[:, tokens // 2 - 1 : tokens // 2]
    total = cum[:, tokens - 1 :]
    before_scale = jnp.exp(mid - cum) * step
    after_scale = jnp.exp(cum - mid)

    def put(first, columns, value):
        high = rounded(value)
        m_ref[first : first + heads, columns] = high
        m_ref[first + 32 : first + 32 + heads, columns] = value - high

    wide = (heads, LANE)
    put(0, slice(0, tokens), before_scale)
    put(64, slice(0, tokens), after_scale)
    put(0, slice(tokens, tokens + LANE), jnp.broadcast_to(jnp.exp(mid), wide))
    put(64, slice(tokens, tokens + LANE), jnp.broadcast_to(skip, wide))
    mt_ref[...] = m_ref[...].T.astype(BF16)
    gate_row = jnp.where(last_start < offset.astype(F32), total, -1e30)
    link_row = jnp.sum(
        jnp.where(
            lax.broadcasted_iota(jnp.int32, (heads, LANE), 0)
            == lax.broadcasted_iota(jnp.int32, (heads, LANE), 1),
            gate_row,
            0.0,
        ),
        axis=0,
        keepdims=True,
    )

    def expand(rows, upper):
        block = mt_ref[rows, :]
        at = lax.broadcasted_iota(jnp.int32, block.shape, 1)
        block = jnp.where((at >= 64) if upper else (at < 64), block.astype(F32), 0.0)
        return block.astype(BF16)

    row_ref[0:8, :] = dot(expand(slice(tokens - 8, tokens), True), e_ref[...])
    row_ref[8:16, :] = dot(expand(slice(tokens, tokens + 8), False), e_ref[...])
    row_ref[16:24, :] = dot(expand(slice(tokens, tokens + 8), True), e_ref[...])

    step_rows = 128
    columns = [slice(c, c + 256) for c in range(0, channels, 256)]
    cuts = [(c, min(256, side_width - c)) for c in range(0, side_width, 256)]
    mine = core * side_width
    others = (1 - core) * side_width

    def lanes(base, cut):
        return pl.ds(pl.multiple_of(base + cut[0], LANE), cut[1])

    loads[1].wait()
    kept = jnp.where(position.astype(F32) >= last_start, b_v[...].astype(F32), 0.0)
    kept = kept.T.astype(BF16)
    loads[2].wait()
    for load in loads[3:]:
        load.start()

    def summary(base, store):
        @pl.loop(0, tokens // step_rows)
        def _(i):
            rows = pl.ds(pl.multiple_of(i * step_rows, step_rows), step_rows)
            left = expand(rows, False)
            for cut in cuts:
                cols = lanes(base, cut)
                v_ref[rows, cols] = (
                    x_v[rows, cols].astype(F32) * dot(left, e_ref[:, cols])
                ).astype(BF16)

        for cut in cuts:
            cols = lanes(base, cut)
            store(
                slice(cut[0], cut[0] + cut[1]),
                dot(kept, v_ref[:, cols]) * row_ref[7:8, cols],
            )

    def to_partner(cols, value):
        pair_send[0:state, cols] = value.astype(BF16)

    def to_own(cols, value):
        own_s[:, cols] = value

    pair_send[state:, :] = jnp.zeros((8, side_width), BF16)
    pair_send[state:, 0:LANE] = link_tile(link_row, 8)
    summary(others, to_partner)
    pl.semaphore_wait(barrier, len(greeted))
    pair = send(pair_send, pair_recv, p_sem.at[0], p_sem.at[1], partner)
    summary(mine, to_own)

    def link_of(block):
        return jnp.sum(block.astype(F32), axis=0, keepdims=True)

    def spread(logs):
        at = lax.broadcasted_iota(jnp.int32, logs.shape, 1)
        value = jnp.where(at < heads, jnp.exp(logs), 0.0)
        high = value.astype(BF16)
        rest = value - high.astype(F32)
        middle = rest.astype(BF16)
        low = (rest - middle.astype(F32)).astype(BF16)
        hot = e_ref[:, pl.ds(pl.multiple_of(mine, LANE), side_width)]
        return dot(high, hot) + dot(middle, hot) + dot(low, hot)

    pair.wait_recv()
    partner_row = link_of(pair_recv[state:, 0:LANE])
    ll_ref[0:1, :] = jnp.where(is_first, link_row, partner_row)
    ll_ref[1:2, :] = jnp.where(is_first, partner_row, link_row)
    chip_log = link_row + partner_row
    pair_links = spread(ll_ref[0:8, :])
    l0_ref[...] = pair_links[0:1, :]
    zlog_send[...] = chip_log
    zlog_copies = {}
    for k in around(nz):
        zlog_copies[k] = send(
            zlog_send, zlog_recv.at[z], la_ssem.at[k - 1], la_rsem.at[k - 1], in_z[k]
        )
    zlog_recv[z] = chip_log
    row_copies = {}
    cut_at = (side_width * 3 // 5) // LANE * LANE
    groups = (slice(0, cut_at), slice(cut_at, side_width))

    def send_out(g, k, slot):
        row_copies[g, k] = send(
            asend.at[slot, :, groups[g]],
            arecv.at[z, :, groups[g]],
            a_ssem.at[g, k - 1],
            a_rsem.at[g, k - 1],
            in_z[k],
        )

    for k in [*around(nz), 0]:
        slot = (z + k) % nz
        rows = pl.ds(pl.multiple_of(slot * sr, sr), sr)
        own = own_s[rows, :]
        came = pair_recv[rows, :].astype(F32)
        earlier_core = jnp.where(is_first, own, came)
        first_s[rows, :] = earlier_core
        merged = pair_links[1:2, :] * earlier_core + jnp.where(is_first, came, own)
        if k:
            asend[slot] = merged.astype(BF16)
            send_out(0, k, slot)
        else:
            arecv[z] = merged.astype(BF16)
    for k in around(nz):
        send_out(1, k, (z + k) % nz)

    loads[3].wait()
    cj_ref[...] = jnp.where(joined, c_v[...].astype(F32), 0.0).astype(BF16)
    loads[4].wait()

    def alone(first):
        rows = pl.ds(first, step_rows)
        scores = dot_nt(c_v[rows, :], b_v[...])
        at = offset + first + lax.broadcasted_iota(jnp.int32, (step_rows, 1), 0)
        source = offset + lax.broadcasted_iota(jnp.int32, (step_rows, tokens), 1)
        begun = jnp.max(
            jnp.where(starts <= at, starts.astype(F32), -1.0), axis=1, keepdims=True
        )
        live = (source <= at) & (source.astype(F32) >= begun)
        sc_ref[...] = jnp.where(live, scores, 0.0).astype(BF16)
        left = expand(rows, True)
        for cols in columns:
            scale = dot(left, e_ref[:, cols])
            gate = g_v[rows, cols].astype(F32)
            gate = gate / (1.0 + jnp.exp(-gate))
            inside = dot(sc_ref[...], v_ref[:, cols])
            skipped = row_ref[16:17, cols] * x_v[rows, cols].astype(F32)
            a1_ref[rows, cols] = scale * gate
            a2_ref[rows, cols] = (scale * inside + skipped) * gate

    @pl.loop(0, tokens // step_rows)
    def _(i):
        alone(pl.multiple_of(i * step_rows, step_rows))

    for k in around(nz):
        zlog_copies[k].wait_recv()
    for j in range(nz):
        ll_ref[j : j + 1, :] = zlog_recv[j]
    row_log = jnp.sum(ll_ref[0:nz, :], axis=0, keepdims=True)
    xlog_send[...] = row_log
    xlog_copies = {}
    for k in around(nx):
        xlog_copies[k] = send(
            xlog_send, xlog_recv.at[xi], lx_ssem.at[k - 1], lx_rsem.at[k - 1], in_x[k]
        )
    xlog_recv[xi] = row_log
    lx_ref[0:nz, :] = spread(ll_ref[0:nz, :])
    x_copies = {}
    for g, cols in enumerate(groups):
        for k in around(nz):
            row_copies[g, k].wait_recv()
        prefix = jnp.zeros((sr, cols.stop - cols.start), F32)
        product = jnp.ones((1, cols.stop - cols.start), F32)
        for j in range(nz):
            pre_ref[j, :, cols] = prefix
            pl_ref[j : j + 1, cols] = product
            link = lx_ref[j : j + 1, cols]
            prefix = link * prefix + arecv[j, :, cols].astype(F32)
            product = product * link
        xsend[:, cols] = prefix.astype(BF16)
        for k in around(nx):
            x_copies[g, k] = send(
                xsend.at[:, cols],
                xrecv.at[xi, :, cols],
                x_ssem.at[g, k - 1],
                x_rsem.at[g, k - 1],
                in_x[k],
            )
        xrecv[xi, :, cols] = xsend[:, cols]
    for k in around(nx):
        xlog_copies[k].wait_recv()
    for j in range(nx):
        ll_ref[j : j + 1, :] = xlog_recv[j]
    lx_ref[0:nx, :] = spread(ll_ref[0:nx, :])
    back_copies = {}
    for g, cols in enumerate(groups):
        for k in around(nx):
            x_copies[g, k].wait_recv()
        earlier = jnp.zeros((sr, cols.stop - cols.start), F32)
        for j in range(nx - 1):
            after = lx_ref[j : j + 1, cols] * earlier + xrecv[j, :, cols].astype(F32)
            earlier = jnp.where(j < xi, after, earlier)
        for k in [*around(nz), 0]:
            slot = (z + k) % nz
            value = (pre_ref[slot, :, cols] + pl_ref[pl.ds(slot, 1), cols] * earlier).astype(BF16)
            if k:
                bsend[slot, :, cols] = value
                back_copies[g, k] = send(
                    bsend.at[slot, :, cols],
                    brecv.at[z, :, cols],
                    b_ssem.at[g, k - 1],
                    b_rsem.at[g, k - 1],
                    in_z[k],
                )
            else:
                brecv[z, :, cols] = value

    final_copies = []
    for g, cols in enumerate(groups):
        own_lanes = pl.ds(pl.multiple_of(mine + cols.start, LANE), cols.stop - cols.start)
        for k in [0] + around(nz)[::-1]:
            if k:
                back_copies[g, k].wait_recv()
            slot = (z + nz - k) % nz
            rows = pl.ds(pl.multiple_of(slot * sr, sr), sr)
            to_first = brecv[slot, :, cols].astype(F32)
            to_second = l0_ref[:, cols] * to_first + first_s[rows, cols]
            fsend[slot, :, cols] = jnp.where(is_first, to_second, to_first).astype(BF16)
            final_copies.append(
                send(
                    fsend.at[slot, :, cols],
                    frecv.at[slot, :, cols],
                    f_ssem.at[g, k],
                    f_rsem.at[g, k],
                    partner,
                )
            )
            sp_ref[rows, own_lanes] = (
                row_ref[8:9, own_lanes] * jnp.where(is_first, to_first, to_second)
            ).astype(BF16)

    sends = [pair]
    for copies in (zlog_copies, row_copies, xlog_copies, x_copies, back_copies):
        sends += copies.values()
    sends += final_copies

    def chunk_rows(k):
        return pl.ds(pl.multiple_of(((head + k) % ny) * part, part), part)

    def hidden_columns(rows, cols):
        gated = a2_ref[rows, cols] + a1_ref[rows, cols] * dot(cj_ref[rows, :], sp_ref[:, cols])
        hid_ref[rows, cols] = (gated * gain_ref[cols].reshape(1, cols.size)).astype(BF16)
        return jnp.sum(gated * gated, axis=1, keepdims=True)

    def share_squares(k, squares):
        ss_send[k] = jnp.broadcast_to(as_row(squares, part), (8, part))
        if k:
            return send(
                ss_send.at[k],
                ss_recv.at[k - 1],
                ss_ssem.at[k - 1],
                ss_rsem.at[k - 1],
                in_y[k],
            )

    def make_hidden(k):
        rows = chunk_rows(k)
        squares = jnp.zeros((part, 1), F32)
        for cols in columns:
            squares = squares + hidden_columns(rows, pl.ds(cols.start, 256))
        return share_squares(k, squares)

    def project(k, base, span, store):
        rows = chunk_rows(k)
        for c in range(span[0], span[1], 256):
            store(
                slice(c, c + 256),
                dot(hid_ref[rows, :], w_v[:, base + c : base + c + 256]),
            )

    def into(ref):
        def store(cols, value):
            ref[:, cols] = value.astype(BF16)

        return store

    def added(ref, extra):
        def store(cols, value):
            ref[:, cols] = (value + extra[:, cols].astype(F32)).astype(BF16)

        return store

    far = chunk_rows(2)
    squares = jnp.zeros((part, 1), F32)
    for cut in cuts:
        squares = squares + hidden_columns(far, lanes(mine, cut))
    for g, cols in enumerate(groups):
        size = cols.stop - cols.start
        for copy in final_copies[g * nz : (g + 1) * nz]:
            copy.wait_recv()
        other_lanes = pl.ds(pl.multiple_of(others + cols.start, LANE), size)
        for j in range(nz):
            rows = slice(j * sr, (j + 1) * sr)
            sp_ref[rows, other_lanes] = (
                row_ref[8:9, other_lanes] * frecv[j, :, cols].astype(F32)
            ).astype(BF16)
        for c in range(0, size, 256):
            cut = (cols.start + c, min(256, size - c))
            squares = squares + hidden_columns(far, lanes(others, cut))
    loads[5].wait()
    up, down = in_y[1], in_y[ny - 1]
    spans = ((0, 256), (256, half))
    last_spans = ((0, half - 256), (half - 256, half))
    first = {}
    for p, span in enumerate(spans):
        for side, device in ((0, up), (1, down)):
            project(2, side * half, span, into(r1_send.at[side]))
            cols = slice(*span)
            first[side, p] = send(
                r1_send.at[side, :, cols],
                r1_recv.at[side, :, cols],
                r1_ssem.at[side, p],
                r1_rsem.at[side, p],
                device,
            )
    squares_sent = [share_squares(2, squares)]
    second = {}
    for side, k, device in ((0, 1, up), (1, ny - 1, down)):
        squares_sent.append(make_hidden(k))
        project(k, (1 - side) * half, (0, half), into(r2_send.at[side, 0]))
        second[side, 0] = send(
            r2_send.at[side, 0],
            r2_recv.at[side, 0],
            r2_ssem.at[side, 0],
            r2_rsem.at[side, 0],
            device,
        )
    make_hidden(0)
    for side in (0, 1):

        def store(cols, value, side=side):
            own_ref[:, side * half + cols.start : side * half + cols.stop] = value

        project(0, side * half, (0, half), store)
    for p, span in enumerate(last_spans):
        for side, k, device in ((0, 1, up), (1, ny - 1, down)):
            if p == 0:
                first[side, 0].wait_recv()
                first[side, 1].wait_recv()
            project(k, side * half, span, added(r2_send.at[side, 1], r1_recv.at[side]))
            cols = slice(*span)
            second[side, 1 + p] = send(
                r2_send.at[side, 1, :, cols],
                r2_recv.at[side, 1, :, cols],
                r2_ssem.at[side, 1 + p],
                r2_rsem.at[side, 1 + p],
                device,
            )
    for copy in squares_sent:
        copy.wait_recv()
    total_squares = ss_send[0]
    for k in range(ny - 1):
        total_squares = total_squares + ss_recv[k]
    scale = lax.rsqrt(as_column(total_squares[0:1, :], part) / DI + EPSILON)
    for side in (0, 1):
        second[side, 0].wait_recv()
        base = (1 - side) * half
        for c in range(0, half, 256):
            cols = slice(base + c, base + c + 256)
            own_ref[:, cols] = own_ref[:, cols] + r2_recv[side, 0, :, c : c + 256].astype(F32)
    for p, span in enumerate(last_spans):
        for side in (0, 1):
            second[side, 1 + p].wait_recv()
            base = side * half
            for c in range(span[0], span[1], 256):
                cols = slice(base + c, base + c + 256)
                value = own_ref[:, cols] + r2_recv[side, 1, :, c : c + 256].astype(F32)
                out_ref[:, cols] = (value * scale).astype(BF16)
    for copy in sends + squares_sent + [*first.values(), *second.values()]:
        copy.wait_send()


def local(nx, nz, ny, stream, gate, inc, outc, step_raw, bias, rate, skip, gain, proj, starts):
    tokens, channels = stream.shape
    heads = step_raw.shape[0]
    state = inc.shape[1]
    width = proj.shape[1]
    half = width // 2
    sw = channels // 2
    sr = state // nz
    part = tokens // ny
    anyspace = pl.BlockSpec(memory_space=pl.ANY)
    dma = pltpu.SemaphoreType.DMA
    scratch = [
        pltpu.VMEM((1, heads), F32),
        pltpu.VMEM((1, heads), F32),
        pltpu.VMEM((1, heads), F32),
        pltpu.VMEM((channels,), F32),
        pltpu.VMEM((1, starts.shape[0]), jnp.int32),
        pltpu.VMEM((tokens, channels), BF16),
        pltpu.VMEM((tokens, channels), BF16),
        pltpu.VMEM((tokens, state), BF16),
        pltpu.VMEM((tokens, state), BF16),
        pltpu.VMEM((heads, tokens), F32),
        pltpu.VMEM((channels, width), BF16),
        pltpu.VMEM((LANE, tokens + LANE), F32),
        pltpu.VMEM((tokens + LANE, LANE), BF16),
        pltpu.VMEM((LANE, channels), BF16),
        pltpu.VMEM((tokens, channels), BF16),
        pltpu.VMEM((128, tokens), BF16),
        pltpu.VMEM((tokens, state), BF16),
        pltpu.VMEM((tokens, channels), F32),
        pltpu.VMEM((tokens, channels), F32),
        pltpu.VMEM((24, channels), F32),
        pltpu.VMEM((state, sw), F32),
        pltpu.VMEM((state + 8, sw), BF16),
        pltpu.VMEM((state + 8, sw), BF16),
        pltpu.VMEM((state, sw), F32),
        pltpu.VMEM((nz, sr, sw), BF16),
        pltpu.VMEM((nz, sr, sw), BF16),
        pltpu.VMEM((1, LANE), F32),
        pltpu.VMEM((nz, 1, LANE), F32),
        pltpu.VMEM((1, LANE), F32),
        pltpu.VMEM((nx, 1, LANE), F32),
        pltpu.VMEM((8, LANE), F32),
        pltpu.VMEM((8, sw), F32),
        pltpu.VMEM((1, sw), F32),
        pltpu.VMEM((nz, sr, sw), F32),
        pltpu.VMEM((8, sw), F32),
        pltpu.VMEM((sr, sw), BF16),
        pltpu.VMEM((nx, sr, sw), BF16),
        pltpu.VMEM((nz, sr, sw), BF16),
        pltpu.VMEM((nz, sr, sw), BF16),
        pltpu.VMEM((nz, sr, sw), BF16),
        pltpu.VMEM((nz, sr, sw), BF16),
        pltpu.VMEM((state, channels), BF16),
        pltpu.VMEM((tokens, channels), BF16),
        pltpu.VMEM((2, part, half), BF16),
        pltpu.VMEM((2, part, half), BF16),
        pltpu.VMEM((2, 2, part, half), BF16),
        pltpu.VMEM((2, 2, part, half), BF16),
        pltpu.VMEM((part, width), F32),
        pltpu.VMEM((ny, 8, part), F32),
        pltpu.VMEM((ny - 1, 8, part), F32),
        dma((5,)),
        dma((6,)),
        dma((2,)),
        dma((nz - 1,)),
        dma((nz - 1,)),
        dma((nx - 1,)),
        dma((nx - 1,)),
        dma((2, nz - 1)),
        dma((2, nz - 1)),
        dma((2, nx - 1)),
        dma((2, nx - 1)),
        dma((2, nz - 1)),
        dma((2, nz - 1)),
        dma((2, nz)),
        dma((2, nz)),
        dma((2, 2)),
        dma((2, 2)),
        dma((2, 3)),
        dma((2, 3)),
        dma((ny - 1,)),
        dma((ny - 1,)),
    ]
    return pl.pallas_call(
        functools.partial(kernel, nx, nz, ny),
        out_shape=pltpu.VMEM((part, width), BF16),
        in_specs=[anyspace] * 11,
        out_specs=pl.BlockSpec(memory_space=pltpu.VMEM),
        scratch_shapes=scratch,
        compiler_params=pltpu.CompilerParams(
            collective_id=0, has_side_effects=True, vmem_limit_bytes=56 * 1024 * 1024
        ),
        name="ssd_layer",
    )(
        stream,
        gate,
        inc,
        outc,
        step_raw,
        bias[None],
        rate[None],
        skip[None],
        gain,
        proj,
        starts[None],
    )


def solution(mesh):
    chips = mesh.shape["seq"] // 2
    nz = min(ALONG_Z, chips)
    in_specs = (
        P("seq", "head"),
        P("seq", "head"),
        P("seq", None),
        P("seq", None),
        P("head", "seq"),
        P("head"),
        P("head"),
        P("head"),
        P("head"),
        P("head", None),
        P(),
    )
    return jax.shard_map(
        functools.partial(local, chips // nz, nz, mesh.shape["head"]),
        mesh=mesh,
        in_specs=in_specs,
        out_specs=P(("seq", "head"), None),
        check_vma=False,
    )
```
